32 devices in a mesh: data: 1 (over z), outer: 4 (over y), expert: 8 (over x, core).
Axes of the slice: x: 4, y: 4, z: 1, core: 2. Of those that a mesh axis runs over, the one named last changes fastest.
The devices are a block of a 4x4x8 slice.
Arguments:
- x: bfloat16 [16384, 2048], P(('data', 'outer', 'expert'))
- wr: bfloat16 [2048, 128], replicated
- idx: int32 [16384, 8], P(('data', 'outer', 'expert'))
- w1: bfloat16 [128, 2048, 768], P(('outer', 'expert'))
- w3: bfloat16 [128, 2048, 768], P(('outer', 'expert'))
- w2: bfloat16 [128, 768, 2048], P(('outer', 'expert'))
Outputs:
- output: bfloat16 [16384, 2048], P(('data', 'outer', 'expert'))
All inputs are finite; a program needn't handle non-finite values.
Results may differ from the reference program's by a relative error of at most 0.0081153.
Values are sent between devices in bfloat16 or wider.
A program may use at most 768 MiB of HBM per device.

```python
import jax
import jax.numpy as jnp
from jax import lax

OUTER = 4
EXPERT = 8
T = 512
D = 2048
FF = 768
E = 128
TOP = 8

N_DEV = OUTER * EXPERT
CAP = 2 * T * TOP // E


def _w(key, shape, scale):
    ks = jax.random.split(key, shape[0])
    return lax.map(lambda kk: (scale * jax.random.normal(kk, shape[1:], jnp.float32)).astype(jnp.bfloat16), ks)


def setup_inputs(seed: int = 0, part: int = 0) -> dict:
    key = jax.random.key(seed)
    kr, k1, k3, k2 = jax.random.split(key, 4)
    kp = jax.random.fold_in(key, part)
    kx, _, _ = jax.random.split(kp, 3)
    kb1, kb2, kb3 = jax.random.split(jax.random.fold_in(kp, 7), 3)
    x = jax.random.normal(kx, (N_DEV * T, D), jnp.float32).astype(jnp.bfloat16)
    wr = (1.5 * D ** -0.5 * jax.random.normal(kr, (D, E), jnp.float32)).astype(jnp.bfloat16)
    w1 = _w(k1, (E, D, FF), D ** -0.5)
    w3 = _w(k3, (E, D, FF), D ** -0.5)
    w2 = _w(k2, (E, FF, D), FF ** -0.5)
    nc = N_DEV * T // E
    rot = jax.random.randint(kb1, (N_DEV,), 0, E, jnp.int32)
    base = jnp.arange(E, dtype=jnp.int32) // 2
    p = jax.vmap(lambda kk: jax.random.permutation(kk, base))(jax.random.split(kb2, nc))
    p = p + jnp.repeat(rot, T // E)[:, None]
    w = min(2 * TOP, E)
    off = jax.vmap(lambda kk: jax.random.permutation(kk, w)[:TOP])(jax.random.split(kb3, nc))
    idx = ((p[:, :, None] + off[:, None, :]) % E).reshape(N_DEV * T, TOP).astype(jnp.int32)
    return {'x': x, 'wr': wr, 'idx': idx, 'w1': w1, 'w3': w3, 'w2': w2}


def _ranks(e, num):
    order = jnp.argsort(e, stable=True)
    se = e[order]
    first = jnp.searchsorted(se, jnp.arange(num, dtype=jnp.int32), side='left').astype(jnp.int32)
    r = jnp.arange(e.shape[0], dtype=jnp.int32) - first[se]
    return jnp.zeros_like(e).at[order].set(r)


def reference(x, wr, idx, w1, w3, w2):
    logits = jnp.dot(x, wr, preferred_element_type=jnp.float32)
    g = jax.nn.softmax(jnp.take_along_axis(logits, idx, axis=1), axis=-1)
    eb = idx.reshape(N_DEV, T * TOP)
    r = jax.vmap(lambda v: _ranks(v, E))(eb).reshape(-1)
    e = eb.reshape(-1)
    src = jnp.arange(N_DEV * T * TOP, dtype=jnp.int32) // (T * TOP)
    tok = jnp.arange(N_DEV * T * TOP, dtype=jnp.int32) // TOP
    pos = jnp.where(r < CAP, e * (N_DEV * CAP) + src * CAP + r, E * N_DEV * CAP)
    tab = jnp.full((E * N_DEV * CAP,), N_DEV * T, jnp.int32).at[pos].set(tok, mode='drop').reshape(E, N_DEV * CAP)
    gt = jnp.zeros((E * N_DEV * CAP,), jnp.float32).at[pos].set(g.reshape(-1), mode='drop').reshape(E, N_DEV * CAP)

    def step(y, inp):
        t, gw, a1, a3, a2 = inp
        xe = jnp.take(x, t, axis=0, mode='fill', fill_value=0)
        a = jnp.dot(xe, a1, preferred_element_type=jnp.float32)
        b = jnp.dot(xe, a3, preferred_element_type=jnp.float32)
        h = (jax.nn.silu(a) * b).astype(jnp.bfloat16)
        o = jnp.dot(h, a2, preferred_element_type=jnp.float32).astype(jnp.bfloat16)
        return y.at[t].add(gw[:, None] * o.astype(jnp.float32), mode='drop'), None

    y, _ = lax.scan(step, jnp.zeros((N_DEV * T, D), jnp.float32), (tab, gt, w1, w3, w2))
    return y.astype(jnp.bfloat16)
```

```python
import functools

import jax
import jax.numpy as jnp
from jax import lax
from jax.experimental import pallas as pl
from jax.experimental.pallas import tpu as pltpu
from jax.sharding import PartitionSpec as P

MESH = pl.DeviceIdType.MESH
F32 = jnp.float32
BF16 = jnp.bfloat16


def _gate(x, wr, idx):
    logits = jnp.dot(x, wr, preferred_element_type=F32)
    oh = idx[:, :, None] == jnp.arange(wr.shape[1], dtype=idx.dtype)
    return jax.nn.softmax(jnp.sum(jnp.where(oh, logits[:, None, :], 0.0), axis=-1), axis=-1)


def _parts(w):
    hi = lax.reduce_precision(w, 8, 7)
    r = w - hi
    mid = lax.reduce_precision(r, 8, 7)
    return hi, mid, r - mid


def _tables(idx, g, E, C):
    t, k = idx.shape
    oh = idx[:, :, None] == jnp.arange(E, dtype=idx.dtype)
    m = jnp.sum(oh, axis=1, dtype=jnp.int32).astype(BF16)
    pos = jnp.arange(t, dtype=jnp.int32)
    tri = (pos[None, :] < pos[:, None]).astype(BF16)
    cnt = jnp.dot(tri, m, preferred_element_type=F32)
    r = jnp.sum(jnp.where(oh, cnt[:, None, :], 0.0), axis=-1)
    ohr = r[:, :, None] == jnp.arange(C, dtype=F32)
    one = jnp.ones((t, k), F32)
    lo = (pos % 256).astype(F32)[:, None] * one
    hi = (pos // 256).astype(F32)[:, None] * one
    vals = jnp.stack((one, hi, lo) + _parts(g), axis=-1)
    rhs = jnp.where(ohr[:, :, None, :], vals[..., None], 0.0).astype(BF16)
    res = jnp.einsum('tje,tjic->iec', oh.astype(BF16), rhs, preferred_element_type=F32)
    tab = jnp.where(res[0] > 0.5, res[1] * 256.0 + res[2], -1.0).astype(jnp.int32)
    return tab, (res[3] + res[4]) + res[5]


def _kernel(O, X, el, C, xall, tab_in, tab_own, g_own, w1, w3, w2, y, stage, recv,
            w1v, w3v, w2v, xs, xt, ob, acc, wsem, xsem, osem, ysem, ssem, rsem):
    n = O * X
    W = X // 2
    T, D = acc.shape
    B = el * C
    G = 2 * W
    NG = n // G
    half = G * C // 2
    mo = lax.axis_index('outer')
    mx = lax.axis_index('expert')
    mc = mx // 2
    core = lax.rem(mx, 2)
    me = mo * X + mx

    def seq(i):
        return lax.rem(2 * i + 1 - 3 * (i // 2) + 4, 4)

    def offs(q, j, c):
        a = seq(j // 2)
        b = seq(lax.rem(j // 2 + q, W))
        return a + c * (b - a), b + c * (a - b)

    def peer(q, j):
        a, b = offs(q, j, core)
        return lax.rem(mo + a, O), 2 * lax.rem(mc + b, W) + lax.rem(core + j % 2, 2)

    def origin(q, j):
        c = lax.rem(core + j % 2, 2)
        a, b = offs(q, j, c)
        return lax.rem(mo - a + O, O), 2 * lax.rem(mc - b + W, W) + c

    def flat(p):
        return p[0] * X + p[1]

    def block(ref, d):
        return ref.at[pl.ds(pl.multiple_of(d * B, B), B)]

    def is_self(q, j):
        return (q == 0) & (j == G - 2)

    bar = pltpu.get_barrier_semaphore()

    def greet(s, _):
        q, j = s // G, lax.rem(s, G)

        @pl.when(jnp.logical_not(is_self(q, j)))
        def _():
            po, px = peer(q, j)
            pl.semaphore_signal(bar, inc=1, device_id={'outer': po, 'expert': px}, device_id_type=MESH)
        return 0

    lax.fori_loop(0, n, greet, 0)

    def wcopies(e):
        return (pltpu.make_async_copy(w1.at[e], w1v.at[e], wsem.at[0, e]),
                pltpu.make_async_copy(w3.at[e], w3v.at[e], wsem.at[1, e]),
                pltpu.make_async_copy(w2.at[e], w2v.at[e], wsem.at[2, e]))

    def xcopy(s, slot):
        src = flat(peer(s // G, lax.rem(s, G)))
        return pltpu.make_async_copy(xall.at[pl.ds(pl.multiple_of(src * T, T), T)], xs.at[slot], xsem.at[slot])

    xcopy(0, 0).start()
    for e in range(el):
        for cp in wcopies(e):
            cp.start()
    pl.semaphore_wait(bar, n - 1)

    def send(q, j):
        po, px = peer(q, j)
        k = q * G + j
        return pltpu.make_async_remote_copy(
            src_ref=block(stage, po * X + px), dst_ref=block(recv, me), send_sem=ssem.at[k],
            recv_sem=rsem.at[k], device_id={'outer': po, 'expert': px}, device_id_type=MESH)

    tok = lax.broadcasted_iota(jnp.int32, (T, B), 0)
    NT = 512

    def group(q, _):
        def pick(j, _):
            s = q * G + j
            slot = lax.rem(s, 2)

            @pl.when(s + 1 < n)
            def _():
                xcopy(s + 1, 1 - slot).start()
            xcopy(s, slot).wait()
            row = tab_in[pl.ds(flat(peer(q, j)), 1), :]
            hot = jnp.where(tok == row, 1.0, 0.0).astype(BF16)
            at = pl.ds(pl.multiple_of(j * C, C), C)
            for c0 in range(0, D, NT):
                r = lax.dot_general(hot, xs[slot, :, c0:c0 + NT], (((0,), (0,)), ((), ())),
                                    preferred_element_type=F32).astype(BF16)
                for e in range(el):
                    xt[e, at, c0:c0 + NT] = r[e * C:(e + 1) * C]
            return 0

        lax.fori_loop(0, G, pick, 0)

        def odrain(slot):
            pltpu.make_async_copy(ob.at[slot], stage.at[pl.ds(0, half)], osem.at[slot]).wait()

        def ffn(i, _):
            e, hh = i // 2, lax.rem(i, 2)

            @pl.when((q == 0) & (hh == 0))
            def _():
                for cp in wcopies(e):
                    cp.wait()
            xr = xt[e, pl.ds(pl.multiple_of(hh * half, half), half), :]
            a = jnp.dot(xr, w1v[e], preferred_element_type=F32)
            b = jnp.dot(xr, w3v[e], preferred_element_type=F32)
            h = (jax.nn.silu(a) * b).astype(BF16)

            @pl.when(i >= 2)
            def _():
                odrain(hh)
            for c0 in range(0, D, NT):
                ob[hh, :, c0:c0 + NT] = jnp.dot(h, w2v[e, :, c0:c0 + NT], preferred_element_type=F32).astype(BF16)
            for jj in range(G // 2):
                d = flat(peer(q, hh * (G // 2) + jj))
                pltpu.make_async_copy(
                    ob.at[hh, pl.ds(jj * C, C)],
                    stage.at[pl.ds(pl.multiple_of(d * B + e * C, C), C)], osem.at[hh]).start()
            return 0

        lax.fori_loop(0, 2 * el, ffn, 0)
        for hh in range(2):
            odrain(hh)

        def go(j, _):
            @pl.when(jnp.logical_not(is_self(q, j)))
            def _():
                send(q, j).start()
            return 0

        lax.fori_loop(0, G, go, 0)
        return 0

    lax.fori_loop(0, NG, group, 0)

    acc[...] = jnp.zeros_like(acc)

    def rcopy(p, i, slot, own):
        q, j = p // W, 2 * lax.rem(p, W) + i
        ref = stage if own else recv
        return pltpu.make_async_copy(block(ref, flat(origin(q, j))), xs.at[slot, pl.ds(i * B, B)], rsem2(slot, i))

    def rsem2(slot, i):
        return ysem.at[2 * slot + i]

    def fetch(p, slot):
        for i in range(2):
            q, j = p // W, 2 * lax.rem(p, W) + i
            k = q * G + j
            if i == 0:
                own = p == W - 1

                @pl.when(own)
                def _():
                    rcopy(p, i, slot, True).start()

                @pl.when(jnp.logical_not(own))
                def _():
                    po, px = origin(q, j)
                    arrive(k, po, px).wait_recv()
                    rcopy(p, i, slot, False).start()
            else:
                po, px = origin(q, j)
                arrive(k, po, px).wait_recv()
                rcopy(p, i, slot, False).start()

    def arrive(k, po, px):
        return pltpu.make_async_remote_copy(
            src_ref=block(stage, po * X + px), dst_ref=block(recv, po * X + px), send_sem=ssem.at[k],
            recv_sem=rsem.at[k], device_id={'outer': po, 'expert': px}, device_id_type=MESH)

    fetch(0, 0)

    def comb(p, _):
        slot = lax.rem(p, 2)

        @pl.when(p + 1 < n // 2)
        def _():
            fetch(p + 1, 1 - slot)
        ws = []
        for i in range(2):
            m = flat(origin(p // W, 2 * lax.rem(p, W) + i))
            w = jnp.where(tok == tab_own[pl.ds(m, 1), :], g_own[pl.ds(m, 1), :], 0.0)
            hi = w.astype(BF16)
            r = w - hi.astype(F32)
            mid = r.astype(BF16)
            lo = (r - mid.astype(F32)).astype(BF16)
            ws.append((hi, mid, lo))
        for i in range(2):
            rcopy(p, i, slot, False).wait()
        lhs = [jnp.concatenate((ws[0][u], ws[1][u]), axis=1) for u in range(3)]
        for c0 in range(0, D, NT):
            rr = xs[slot, :, c0:c0 + NT]
            acc[:, c0:c0 + NT] += (jnp.dot(lhs[0], rr, preferred_element_type=F32)
                                   + jnp.dot(lhs[1], rr, preferred_element_type=F32)
                                   + jnp.dot(lhs[2], rr, preferred_element_type=F32))
        return 0

    lax.fori_loop(0, n // 2, comb, 0)

    ycopies = []
    for hh in range(T // half):
        ob[hh] = acc[hh * half:(hh + 1) * half, :].astype(BF16)
        cp = pltpu.make_async_copy(ob.at[hh], y.at[pl.ds(hh * half, half)], osem.at[hh])
        cp.start()
        ycopies.append(cp)
    for cp in ycopies:
        cp.wait()

    def sent(s, _):
        q, j = s // G, lax.rem(s, G)

        @pl.when(jnp.logical_not(is_self(q, j)))
        def _():
            send(q, j).wait_send()
        return 0

    lax.fori_loop(0, n, sent, 0)


def solution(mesh):
    O = mesh.shape['outer']
    X = mesh.shape['expert']
    n = O * X
    tok = P(('data', 'outer', 'expert'), None)
    wsp = P(('outer', 'expert'), None, None)

    def local(x, wr, idx, w1, w3, w2):
        T, D = x.shape
        k = idx.shape[1]
        E = wr.shape[1]
        el, _, FF = w1.shape
        C = 2 * T * k // E
        B = el * C
        half = X * C // 2
        xall = lax.all_gather(x, ('outer', 'expert'), axis=0, tiled=True)
        g = _gate(x, wr, idx)
        tab, gs = _tables(idx, g, E, C)
        tab_own = tab.reshape(n, B)
        g_own = gs.reshape(n, B)
        tab_in = lax.all_to_all(tab_own, ('outer', 'expert'), 0, 0, tiled=True)
        anyspec = pl.BlockSpec(memory_space=pl.ANY)
        vspec = pl.BlockSpec(memory_space=pltpu.VMEM)
        y, _, _ = pl.pallas_call(
            functools.partial(_kernel, O, X, el, C),
            out_shape=(jax.ShapeDtypeStruct((T, D), BF16),
                       jax.ShapeDtypeStruct((n * B, D), BF16),
                       jax.ShapeDtypeStruct((n * B, D), BF16)),
            in_specs=[anyspec, vspec, vspec, vspec, anyspec, anyspec, anyspec],
            out_specs=(anyspec, anyspec, anyspec),
            scratch_shapes=[
                pltpu.VMEM((el, D, FF), BF16),
                pltpu.VMEM((el, D, FF), BF16),
                pltpu.VMEM((el, FF, D), BF16),
                pltpu.VMEM((2, T, D), BF16),
                pltpu.VMEM((el, X * C, D), BF16),
                pltpu.VMEM((2, half, D), BF16),
                pltpu.VMEM((T, D), F32),
                pltpu.SemaphoreType.DMA((3, el)),
                pltpu.SemaphoreType.DMA((2,)),
                pltpu.SemaphoreType.DMA((2,)),
                pltpu.SemaphoreType.DMA((4,)),
                pltpu.SemaphoreType.DMA((n,)),
                pltpu.SemaphoreType.DMA((n,)),
            ],
            compiler_params=pltpu.CompilerParams(
                collective_id=0, has_side_effects=True, vmem_limit_bytes=67043328),
        )(xall, tab_in, tab_own, g_own, w1, w3, w2)
        return y

    return jax.shard_map(local, mesh=mesh, in_specs=(tok, P(None, None), tok, wsp, wsp, wsp), out_specs=tok, check_vma=False)
```

```python
import functools

import jax
import jax.numpy as jnp
from jax import lax
from jax.experimental import pallas as pl
from jax.experimental.pallas import tpu as pltpu
from jax.sharding import PartitionSpec as P

MESH = pl.DeviceIdType.MESH
F32 = jnp.float32
BF16 = jnp.bfloat16


def _gate(x, wr, idx):
    logits = jnp.dot(x, wr, preferred_element_type=F32)
    oh = idx[:, :, None] == jnp.arange(wr.shape[1], dtype=idx.dtype)
    return jax.nn.softmax(jnp.sum(jnp.where(oh, logits[:, None, :], 0.0), axis=-1), axis=-1)


def _parts(w):
    hi = lax.reduce_precision(w, 8, 7)
    r = w - hi
    mid = lax.reduce_precision(r, 8, 7)
    return hi, mid, r - mid


def _tables(idx, g, E, C):
    t, k = idx.shape
    oh = idx[:, :, None] == jnp.arange(E, dtype=idx.dtype)
    m = jnp.sum(oh, axis=1, dtype=jnp.int32).astype(BF16)
    pos = jnp.arange(t, dtype=jnp.int32)
    tri = (pos[None, :] < pos[:, None]).astype(BF16)
    cnt = jnp.dot(tri, m, preferred_element_type=F32)
    r = jnp.sum(jnp.where(oh, cnt[:, None, :], 0.0), axis=-1)
    ohr = r[:, :, None] == jnp.arange(C, dtype=F32)
    one = jnp.ones((t, k), F32)
    lo = (pos % 256).astype(F32)[:, None] * one
    hi = (pos // 256).astype(F32)[:, None] * one
    vals = jnp.stack((one, hi, lo) + _parts(g), axis=-1)
    rhs = jnp.where(ohr[:, :, None, :], vals[..., None], 0.0).astype(BF16)
    res = jnp.einsum('tje,tjic->iec', oh.astype(BF16), rhs, preferred_element_type=F32)
    tab = jnp.where(res[0] > 0.5, res[1] * 256.0 + res[2], -1.0).astype(jnp.int32)
    return tab, (res[3] + res[4]) + res[5]


def _kernel(O, X, el, C, xall, tab_in, pk_a, pk_b, w1, w3, w2, y, stage, recv, part,
            xs, ob, wsem, xsem, osem, ssem, rsem, pssem, prsem):
    n = O * X
    W = X // 2
    _, T, D = xs.shape
    H = D // 2
    FF = w1.shape[2]
    B = el * C
    G = 2 * W
    NG = n // G
    half = G * C // 2
    NT = 512
    mo = lax.axis_index('outer')
    mx = lax.axis_index('expert')
    mc = mx // 2
    core = lax.rem(mx, 2)

    def offs(q, i):
        u, v = lax.rem(i, 2), lax.rem(i // 2, 2)
        return 1 - q // 2 + 2 * u, 1 - lax.rem(q, 2) + 2 * lax.rem(u + v, 2)

    def dest(q, j):
        a, b = offs(q, j // 2)
        return lax.rem(mo + a, O), lax.rem(mc + b, W), lax.rem(core + j % 2, 2)

    def block(ref, d):
        return ref.at[pl.ds(pl.multiple_of(d * B, B), B)]

    def at_a(yd, sx):
        return yd * X + sx

    def at_b(xd, sy, sc):
        return xd * X + sy * 2 + sc

    bar = pltpu.get_barrier_semaphore()

    def greet(po, px):
        pl.semaphore_signal(bar, inc=1, device_id={'outer': po, 'expert': px}, device_id_type=MESH)

    for d in range(1, X):
        greet(mo, lax.rem(mx + d, X))
    for a in range(1, O):
        for c in range(2):
            greet(lax.rem(mo + a, O), 2 * mc + c)

    def xcopy(s, slot):
        yd, xd, cd = dest(s // G, lax.rem(s, G))
        src = yd * X + 2 * xd + cd
        return pltpu.make_async_copy(xall.at[pl.ds(pl.multiple_of(src * T, T), T)], xs.at[slot], xsem.at[slot])

    def send_a(q, j):
        yd, xd, cd = dest(q, j)
        return pltpu.make_async_remote_copy(
            src_ref=block(stage.at[0], yd * X + 2 * xd + cd), dst_ref=block(recv.at[0], at_a(yd, mx)),
            send_sem=ssem.at[0, q * G + j], recv_sem=rsem.at[0, q * G + j],
            device_id={'outer': mo, 'expert': 2 * xd + cd}, device_id_type=MESH)

    def send_b(q, j):
        yd, xd, cd = dest(q, j)
        return pltpu.make_async_remote_copy(
            src_ref=block(stage.at[1], yd * X + 2 * xd + cd), dst_ref=block(recv.at[1], at_b(xd, mo, core)),
            send_sem=ssem.at[1, q * G + j], recv_sem=rsem.at[1, q * G + j],
            device_id={'outer': yd, 'expert': 2 * mc + cd}, device_id_type=MESH)

    def away(q, j):
        a, b = offs(q, j // 2)
        k = j % 2
        return b + k > 0, a + k > 0

    def experts(w1v, w3v, w2v, xt):
        def wcopies(e):
            return (pltpu.make_async_copy(w1.at[e], w1v.at[e], wsem.at[0, e]),
                    pltpu.make_async_copy(w3.at[e], w3v.at[e], wsem.at[1, e]),
                    pltpu.make_async_copy(w2.at[e], w2v.at[e], wsem.at[2, e]))

        xcopy(0, 0).start()
        for e in range(el):
            for cp in wcopies(e):
                cp.start()
        pl.semaphore_wait(bar, X - 1 + 2 * (O - 1))
        tok = lax.broadcasted_iota(jnp.int32, (T, B), 0)

        def group(q, _):
            def pick(j, _):
                s = q * G + j
                slot = lax.rem(s, 2)

                @pl.when(s + 1 < n)
                def _():
                    xcopy(s + 1, 1 - slot).start()
                xcopy(s, slot).wait()
                yd, xd, cd = dest(q, j)
                row = tab_in[pl.ds(yd * X + 2 * xd + cd, 1), :]
                hot = jnp.where(tok == row, 1.0, 0.0).astype(BF16)
                at = pl.ds(pl.multiple_of(j * C, C), C)
                for c0 in range(0, D, NT):
                    r = lax.dot_general(hot, xs[slot, :, c0:c0 + NT], (((0,), (0,)), ((), ())),
                                        preferred_element_type=F32).astype(BF16)
                    for e in range(el):
                        xt[e, at, c0:c0 + NT] = r[e * C:(e + 1) * C]
                return 0

            lax.fori_loop(0, G, pick, 0)

            def odrain(hh):
                for v in range(2):
                    pltpu.make_async_copy(ob.at[hh, :, pl.ds(v * H, H)], stage.at[v, pl.ds(0, half)],
                                          osem.at[hh, v]).wait()

            def ffn(i, _):
                e, hh = i // 2, lax.rem(i, 2)

                @pl.when((q == 0) & (hh == 0))
                def _():
                    for cp in wcopies(e):
                        cp.wait()
                xr = xt[e, pl.ds(pl.multiple_of(hh * half, half), half), :]
                a = jnp.dot(xr, w1v[e], preferred_element_type=F32)
                b = jnp.dot(xr, w3v[e], preferred_element_type=F32)
                h = (jax.nn.silu(a) * b).astype(BF16)

                @pl.when(i >= 2)
                def _():
                    odrain(hh)
                for c0 in range(0, D, NT):
                    ob[hh, :, c0:c0 + NT] = jnp.dot(h, w2v[e, :, c0:c0 + NT],
                                                    preferred_element_type=F32).astype(BF16)
                for jj in range(G // 2):
                    yd, xd, cd = dest(q, hh * (G // 2) + jj)
                    at = pl.ds(pl.multiple_of((yd * X + 2 * xd + cd) * B + e * C, C), C)
                    for v in range(2):
                        pltpu.make_async_copy(ob.at[hh, pl.ds(jj * C, C), pl.ds(v * H, H)],
                                              stage.at[v, at], osem.at[hh, v]).start()
                return 0

            lax.fori_loop(0, 2 * el, ffn, 0)
            for hh in range(2):
                odrain(hh)

            def go(j, _):
                far_a, far_b = away(q, j)

                @pl.when(far_a)
                def _():
                    send_a(q, j).start()

                @pl.when(far_b)
                def _():
                    send_b(q, j).start()
                return 0

            lax.fori_loop(0, G, go, 0)
            return 0

        lax.fori_loop(0, NG, group, 0)

    pl.run_scoped(experts, pltpu.VMEM((el, D, FF), BF16), pltpu.VMEM((el, D, FF), BF16),
                  pltpu.VMEM((el, FF, D), BF16), pltpu.VMEM((el, G * C, D), BF16))

    def combine(pa, pb):
        pa[...] = jnp.zeros_like(pa)
        pb[...] = jnp.zeros_like(pb)
        tokf = lax.broadcasted_iota(jnp.int32, (T, 2 * B), 0).astype(F32)

        def origins(p):
            a, b = offs(p // W, lax.rem(p, W))
            return a, b, lax.rem(mo - a + O, O), lax.rem(mc - b + W, W)

        def fetch(p, slot):
            a, b, sy, sx = origins(p)
            yd, xd = lax.rem(mo + a, O), lax.rem(mc + b, W)
            for k in range(2):
                q, j = p // W, 2 * lax.rem(p, W) + k
                c = lax.rem(core + k, 2)
                at = pl.ds(pl.multiple_of(c * B, B), B)
                for v in range(2):
                    if v == 0:
                        src, own = block(recv.at[0], at_a(yd, 2 * sx + c)), block(stage.at[0], yd * X + 2 * mc + core)
                    else:
                        src, own = block(recv.at[1], at_b(xd, sy, c)), block(stage.at[1], mo * X + 2 * xd + core)
                    far = (b if v == 0 else a) > 0

                    def bring(ref, v=v, at=at):
                        pltpu.make_async_copy(ref, xs.at[slot, at, pl.ds(v * H, H)], xsem.at[slot]).start()

                    def take(src=src, v=v, j=j, bring=bring):
                        pltpu.make_async_remote_copy(
                            src_ref=src, dst_ref=src, send_sem=ssem.at[v, q * G + j],
                            recv_sem=rsem.at[v, q * G + j],
                            device_id={'outer': mo, 'expert': lax.rem(mx + 1, X)},
                            device_id_type=MESH).wait_recv()
                        bring(src)
                    if k == 1:
                        take()
                    else:
                        pl.when(far)(take)
                        pl.when(jnp.logical_not(far))(functools.partial(bring, own))

        def psend(v, d):
            if v == 0:
                src, to = pa.at[d], {'outer': lax.rem(mo + d, O), 'expert': mx}
            else:
                src, to = pb.at[d], {'outer': mo, 'expert': 2 * lax.rem(mc + d, W) + core}
            return pltpu.make_async_remote_copy(
                src_ref=src, dst_ref=part.at[v, d - 1], send_sem=pssem.at[v, d - 1],
                recv_sem=prsem.at[v, d - 1], device_id=to, device_id_type=MESH)

        fetch(0, 0)

        def weights(ref, d, r0):
            out = []
            rows = [ref[d, 0, pl.ds(r0 + c, 1), :] for c in range(2)]
            gs = [ref[d, 1, pl.ds(r0 + c, 1), :] for c in range(2)]
            w = jnp.where(tokf == jnp.concatenate(rows, axis=1), jnp.concatenate(gs, axis=1), 0.0)
            hi = w.astype(BF16)
            r = w - hi.astype(F32)
            mid = r.astype(BF16)
            return hi, mid, (r - mid.astype(F32)).astype(BF16)

        def comb(p, _):
            slot = lax.rem(p, 2)

            @pl.when(p + 1 < n // 2)
            def _():
                fetch(p + 1, 1 - slot)
            a, b, sy, sx = origins(p)
            wa = weights(pk_a, lax.rem(mo + a, O), 2 * sx)
            wb = weights(pk_b, 2 * lax.rem(mc + b, W) + core, 2 * sy)
            pltpu.make_async_copy(xall.at[pl.ds(0, T)], xs.at[slot], xsem.at[slot]).wait()
            for acc, d, ws, base in ((pa, a, wa, 0), (pb, b, wb, H)):
                for c0 in range(0, H, NT):
                    rr = xs[slot, :, base + c0:base + c0 + NT]
                    acc[d, :, c0:c0 + NT] += (jnp.dot(ws[0], rr, preferred_element_type=F32)
                                              + jnp.dot(ws[1], rr, preferred_element_type=F32)
                                              + jnp.dot(ws[2], rr, preferred_element_type=F32))
            for last, v, ds in ((2 * W - 1, 0, (1, 3)), (3 * W - 1, 1, (1, 3)), (4 * W - 1, 0, (2,)), (4 * W - 1, 1, (2,))):
                @pl.when(p == last)
                def _(v=v, ds=ds):
                    for d in ds:
                        psend(v, d).start()
            return 0

        lax.fori_loop(0, n // 2, comb, 0)

        def sent(s, _):
            q, j = s // G, lax.rem(s, G)
            far_a, far_b = away(q, j)

            @pl.when(far_a)
            def _():
                send_a(q, j).wait_send()

            @pl.when(far_b)
            def _():
                send_b(q, j).wait_send()
            return 0

        lax.fori_loop(0, n, sent, 0)

        accs = (pa, pb)
        for d in (1, 3, 2):
            for v in range(2):
                psend(v, d).wait()
                pltpu.make_async_copy(part.at[v, d - 1], accs[v].at[d], prsem.at[v, d - 1]).start()
            for v in range(2):
                pltpu.make_async_copy(part.at[v, d - 1], accs[v].at[d], prsem.at[v, d - 1]).wait()
                if d != 2:
                    accs[v][0] += accs[v][d]
        for v in range(2):
            for hh in range(T // half):
                rows = slice(hh * half, (hh + 1) * half)
                ob[hh, :, v * H:(v + 1) * H] = (accs[v][0, rows] + accs[v][2, rows]).astype(BF16)
        cps = [pltpu.make_async_copy(ob.at[hh], y.at[pl.ds(hh * half, half)], osem.at[hh, 0])
               for hh in range(T // half)]
        for cp in cps:
            cp.start()
        for cp in cps:
            cp.wait()

    pl.run_scoped(combine, pltpu.VMEM((O, T, H), F32), pltpu.VMEM((W, T, H), F32))


def solution(mesh):
    O = mesh.shape['outer']
    X = mesh.shape['expert']
    n = O * X
    tok = P(('data', 'outer', 'expert'), None)
    wsp = P(('outer', 'expert'), None, None)

    def local(x, wr, idx, w1, w3, w2):
        T, D = x.shape
        k = idx.shape[1]
        E = wr.shape[1]
        el, _, FF = w1.shape
        C = 2 * T * k // E
        B = el * C
        half = X * C // 2
        xall = lax.all_gather(x, ('outer', 'expert'), axis=0, tiled=True)
        g = _gate(x, wr, idx)
        tab, gs = _tables(idx, g, E, C)
        tab_in = lax.all_to_all(tab.reshape(n, B), ('outer', 'expert'), 0, 0, tiled=True)
        pk = jnp.stack((tab.astype(F32).reshape(n, B), gs.reshape(n, B)))
        pk_a = lax.all_to_all(pk.reshape(2, O, X, B).transpose(1, 0, 2, 3), 'outer', 0, 0, tiled=True)
        pk_b = pk.reshape(2, O, X // 2, 2, B).transpose(2, 0, 1, 3, 4).reshape(X // 2, 1, 2, 2 * O, B)
        pk_b = jnp.broadcast_to(pk_b, (X // 2, 2, 2, 2 * O, B)).reshape(X, 2, 2 * O, B)
        pk_b = lax.all_to_all(pk_b, 'expert', 0, 0, tiled=True)
        anyspec = pl.BlockSpec(memory_space=pl.ANY)
        vspec = pl.BlockSpec(memory_space=pltpu.VMEM)
        y = pl.pallas_call(
            functools.partial(_kernel, O, X, el, C),
            out_shape=(jax.ShapeDtypeStruct((T, D), BF16),
                       jax.ShapeDtypeStruct((2, n * B, D // 2), BF16),
                       jax.ShapeDtypeStruct((2, n * B, D // 2), BF16),
                       jax.ShapeDtypeStruct((2, O - 1, T, D // 2), F32)),
            in_specs=[anyspec, vspec, vspec, vspec, anyspec, anyspec, anyspec],
            out_specs=(anyspec,) * 4,
            scratch_shapes=[
                pltpu.VMEM((2, T, D), BF16),
                pltpu.VMEM((2, half, D), BF16),
                pltpu.SemaphoreType.DMA((3, el)),
                pltpu.SemaphoreType.DMA((2,)),
                pltpu.SemaphoreType.DMA((2, 2)),
                pltpu.SemaphoreType.DMA((2, n)),
                pltpu.SemaphoreType.DMA((2, n)),
                pltpu.SemaphoreType.DMA((2, O - 1)),
                pltpu.SemaphoreType.DMA((2, O - 1)),
            ],
            compiler_params=pltpu.CompilerParams(
                collective_id=0, has_side_effects=True, vmem_limit_bytes=67043328),
        )(xall, tab_in, pk_a, pk_b, w1, w3, w2)
        return y[0]

    return jax.shard_map(local, mesh=mesh, in_specs=(tok, P(None, None), tok, wsp, wsp, wsp), out_specs=tok, check_vma=False)
```

```python
import functools

import jax
import jax.numpy as jnp
from jax import lax
from jax.experimental import pallas as pl
from jax.experimental.pallas import tpu as pltpu
from jax.sharding import PartitionSpec as P

MESH = pl.DeviceIdType.MESH
F32 = jnp.float32
BF16 = jnp.bfloat16


def _gate(x, wr, idx):
    logits = jnp.dot(x, wr, preferred_element_type=F32)
    oh = idx[:, :, None] == jnp.arange(wr.shape[1], dtype=idx.dtype)
    return jax.nn.softmax(jnp.sum(jnp.where(oh, logits[:, None, :], 0.0), axis=-1), axis=-1)


def _parts(w):
    hi = lax.reduce_precision(w, 8, 7)
    r = w - hi
    mid = lax.reduce_precision(r, 8, 7)
    return hi, mid, r - mid


def _tables(idx, g, E, C):
    t, k = idx.shape
    oh = idx[:, :, None] == jnp.arange(E, dtype=idx.dtype)
    m = jnp.sum(oh, axis=1, dtype=jnp.int32).astype(BF16)
    pos = jnp.arange(t, dtype=jnp.int32)
    tri = (pos[None, :] < pos[:, None]).astype(BF16)
    cnt = jnp.dot(tri, m, preferred_element_type=F32)
    r = jnp.sum(jnp.where(oh, cnt[:, None, :], 0.0), axis=-1)
    ohr = r[:, :, None] == jnp.arange(C, dtype=F32)
    one = jnp.ones((t, k), F32)
    lo = (pos % 256).astype(F32)[:, None] * one
    hi = (pos // 256).astype(F32)[:, None] * one
    vals = jnp.stack((one, hi, lo) + _parts(g), axis=-1)
    rhs = jnp.where(ohr[:, :, None, :], vals[..., None], 0.0).astype(BF16)
    res = jnp.einsum('tje,tjic->iec', oh.astype(BF16), rhs, preferred_element_type=F32)
    tab = jnp.where(res[0] > 0.5, res[1] * 256.0 + res[2], -1.0).astype(jnp.int32)
    return tab, (res[3] + res[4]) + res[5]


ORDER = ((0, 1), (0, 3), (1, 0), (3, 0), (0, 0), (0, 2), (1, 1), (3, 3),
         (1, 3), (3, 1), (1, 2), (3, 2), (2, 1), (2, 3), (2, 0), (2, 2))


def _lut(vals, i):
    r = vals[0]
    for k in range(1, len(vals)):
        r = jnp.where(i == k, vals[k], r)
    return r


def _relays(h, off):
    u, v = off
    if v == 0:
        if u == 3:
            return ((0, 1, 0), (1, 1, None), (1, 3, None))
        if u == 1:
            return ((0, 3, 1), (1, 1, None), (1, 3, None))
        return ((1, 1, None), (1, 3, None))
    if v == 3:
        return ((1, 1, 0),)
    if v == 1:
        return ((1, 3, 1),)
    return ()


def _numbered():
    full, piece = {}, {}
    for h in range(2):
        for d in (1, 3):
            for axis in range(2):
                full[(h, (0, 0), axis, d)] = len(full)
        for u in range(4):
            for v in range(4):
                if (u, v) != (0, 0):
                    for axis, d, part in _relays(h, (u, v)):
                        table = full if part is None else piece
                        table[(h, (u, v), axis, d)] = len(table)
    return full, piece


FULL, PIECE = _numbered()


def _kernel(O, X, el, C, x, pk, w1, w3, w2, y, xall, stage, recv, part,
            xs, ob, tab_in, pk_a, pk_b, wsem, xsem, osem, ssem, rsem, pssem, prsem,
            bsem, bpsem, gsem, gpsem, dsem, hsem, tsem, tsem2):
    n = O * X
    W = X // 2
    _, T, D = xs.shape
    H = D // 2
    FF = w1.shape[2]
    B = el * C
    G = 4
    NG = n // G
    half = G * C
    NT = 512
    mo = lax.axis_index('outer')
    mx = lax.axis_index('expert')
    mc = mx // 2
    core = lax.rem(mx, 2)
    me = mo * X + mx

    def offs(p):
        return _lut([o[0] for o in ORDER], p), _lut([o[1] for o in ORDER], p)

    def dest(s):
        a, b = offs(s // 2)
        return lax.rem(mo + a, O), lax.rem(mc + b, W), lax.rem(core + lax.rem(s, 2), 2)

    def block(ref, d):
        return ref.at[pl.ds(pl.multiple_of(d * B, B), B)]

    def at_a(yd, sx):
        return yd * X + sx

    def at_b(xd, sy, sc):
        return xd * X + sy * 2 + sc

    bar = pltpu.get_barrier_semaphore()

    def greet(d, _):
        t = lax.rem(me + d, n)
        pl.semaphore_signal(bar, inc=1, device_id={'outer': t // X, 'expert': lax.rem(t, X)}, device_id_type=MESH)
        return 0

    lax.fori_loop(1, n, greet, 0)

    def rows(ref, a, b, h, piece, c=None):
        src = lax.rem(mo + a, O) * X + 2 * lax.rem(mc + b, W) + (core if c is None else c)
        step = T // 2
        if piece is None:
            return ref.at[pl.ds(pl.multiple_of(src * T + h * step, step), step)]
        return ref.at[pl.ds(pl.multiple_of(src * T + h * step + piece * (step // 2), step // 2), step // 2)]

    def neighbour(h, axis, d):
        if (axis == 0) == (h == 0):
            return {'outer': mo, 'expert': 2 * lax.rem(mc + d, W) + core}
        return {'outer': lax.rem(mo + d, O), 'expert': mx}

    def offset(h, off):
        return (off[1], off[0]) if h == 0 else off

    def relay(h, off, axis, d, piece, src=None):
        a, b = offset(h, off)
        key = (h, off, axis, d)
        send = gsem.at[FULL[key]] if piece is None else gpsem.at[PIECE[key]]
        u, v = off
        seen = ((u - d) % 4, v) if axis == 0 else (u, (v - d) % 4)
        ra, rb = offset(h, seen)
        k = h * 16 + ra * 4 + rb
        recv_ = bsem.at[k] if piece is None else bpsem.at[2 * k + piece]
        dst = rows(xall, a, b, h, piece)
        pltpu.make_async_remote_copy(src_ref=dst if src is None else src, dst_ref=dst, send_sem=send, recv_sem=recv_,
                                     device_id=neighbour(h, axis, d), device_id_type=MESH).start()

    def share(h, off, src=None):
        a, b = offset(h, off)
        dst = rows(xall, a, b, h, None)
        pltpu.make_async_remote_copy(
            src_ref=dst if src is None else src, dst_ref=dst, send_sem=hsem.at[h * 16 + a * 4 + b],
            recv_sem=dsem.at[a * 4 + b], device_id={'outer': mo, 'expert': 2 * mc + 1 - core},
            device_id_type=MESH).start()

    def other():
        return {'outer': mo, 'expert': 2 * mc + 1 - core}

    def arrive(ref, sem):
        pltpu.make_async_remote_copy(src_ref=ref, dst_ref=ref, send_sem=hsem.at[0], recv_sem=sem,
                                     device_id=other(), device_id_type=MESH).wait_recv()

    def event(h, off):
        a, b = offset(h, off)
        k = h * 16 + a * 4 + b
        if off[1] == 2 or off == (2, 0):
            for piece in range(2):
                arrive(rows(xall, a, b, h, piece), bpsem.at[2 * k + piece])
        else:
            arrive(rows(xall, a, b, h, None), bsem.at[k])
        for axis, d, piece in _relays(h, off):
            relay(h, off, axis, d, piece)
        share(h, off)

    def xcopy(s, slot):
        yd, xd, cd = dest(s)
        at = pl.ds(pl.multiple_of((yd * X + 2 * xd + cd) * T, T), T)
        return pltpu.make_async_copy(xall.at[at], xs.at[slot], xsem.at[slot])

    def xstart(s, slot):
        a, b = offs(s // 2)
        kk = lax.rem(s, 2)
        mine = (a + b + kk) == 0

        @pl.when(kk == 1)
        def _():
            yd, xd, cd = dest(s)
            at = pl.ds(pl.multiple_of((yd * X + 2 * xd + cd) * T, T), T)
            arrive(xall.at[at], dsem.at[a * 4 + b])

        @pl.when(mine)
        def _():
            pltpu.make_async_copy(x, xs.at[slot], xsem.at[slot]).start()

        @pl.when(jnp.logical_not(mine))
        def _():
            xcopy(s, slot).start()

    def send_a(s):
        yd, xd, cd = dest(s)
        return pltpu.make_async_remote_copy(
            src_ref=block(stage.at[0], yd * X + 2 * xd + cd), dst_ref=block(recv.at[0], at_a(yd, mx)),
            send_sem=ssem.at[0, s], recv_sem=rsem.at[0, s],
            device_id={'outer': mo, 'expert': 2 * xd + cd}, device_id_type=MESH)

    def send_b(s):
        yd, xd, cd = dest(s)
        return pltpu.make_async_remote_copy(
            src_ref=block(stage.at[1], yd * X + 2 * xd + cd), dst_ref=block(recv.at[1], at_b(xd, mo, core)),
            send_sem=ssem.at[1, s], recv_sem=rsem.at[1, s],
            device_id={'outer': yd, 'expert': 2 * mc + cd}, device_id_type=MESH)

    def away(s):
        a, b = offs(s // 2)
        k = lax.rem(s, 2)
        return b + k > 0, a + k > 0

    def experts(w1v, w3v, w2v, xt):
        def wcopies(e):
            return (pltpu.make_async_copy(w1.at[e], w1v.at[e], wsem.at[0, e]),
                    pltpu.make_async_copy(w3.at[e], w3v.at[e], wsem.at[1, e]),
                    pltpu.make_async_copy(w2.at[e], w2v.at[e], wsem.at[2, e]))

        pl.semaphore_wait(bar, n - 1)
        step = T // 2
        for h in (0, 1):
            own = x.at[pl.ds(h * step, step)]
            for d in (1, 3):
                relay(h, (0, 0), 0, d, None, own)
        for h in (0, 1):
            own = x.at[pl.ds(h * step, step)]
            for d in (1, 3):
                relay(h, (0, 0), 1, d, None, own)
        for h in (0, 1):
            share(h, (0, 0), x.at[pl.ds(h * step, step)])

        def tell(d, _):
            t = lax.rem(me + d, n)
            to, tx = t // X, lax.rem(t, X)
            pltpu.make_async_remote_copy(
                src_ref=pk.at[0, to, tx], dst_ref=tab_in.at[me], send_sem=tsem.at[0], recv_sem=tsem.at[1],
                device_id={'outer': to, 'expert': tx}, device_id_type=MESH).start()
            return 0

        lax.fori_loop(1, n, tell, 0)
        pltpu.make_async_copy(pk.at[0, mo, mx], tab_in.at[me], tsem2.at[0, 0]).start()
        for d in range(4):
            yo, xo = lax.rem(mo + d, O), lax.rem(mc + d, W)
            if d == 0:
                pltpu.make_async_copy(pk.at[:, mo], pk_a.at[mo], tsem2.at[1, 0]).start()
                pltpu.make_async_copy(pk.at[:, :, pl.ds(2 * mc, 2)], pk_b.at[mc], tsem2.at[2, 0]).start()
            else:
                tsend(0, d).start()
                tsend(1, d).start()
        for e in range(el):
            for cp in wcopies(e):
                cp.start()
        tok = lax.broadcasted_iota(jnp.int32, (T, B), 0).astype(F32)

        for h in (0, 1):
            for u in (1, 3):
                event(h, (u, 0))
        for h in (0, 1):
            for v in (1, 3):
                event(h, (0, v))
        pltpu.make_async_copy(pk.at[0, mo, mx], tab_in.at[me], tsem2.at[0, 0]).wait()
        allrows = pltpu.make_async_remote_copy(
            src_ref=tab_in.at[pl.ds(0, n - 1)], dst_ref=tab_in.at[pl.ds(0, n - 1)], send_sem=tsem.at[0],
            recv_sem=tsem.at[1], device_id=other(), device_id_type=MESH)
        allrows.wait_recv()

        diag = [(h, (u, v)) for u in (1, 3) for v in (1, 3) for h in (0, 1)]
        plan = {0: [(0, (2, 0))], 1: [(1, (2, 0))], 3: [(0, (0, 2))], 4: [(1, (0, 2))],
                5: diag[0:2], 6: diag[2:4], 8: diag[4:6], 9: diag[6:8],
                12: [(0, (2, 1)), (1, (2, 1))], 13: [(0, (2, 3)), (1, (2, 3))],
                15: [(0, (1, 2)), (1, (1, 2))], 16: [(0, (3, 2)), (1, (3, 2))],
                20: [(0, (2, 2)), (1, (2, 2))]}

        xstart(0, 0)

        def group(g, _):
            def pick(j, _):
                s = g * G + j
                slot = lax.rem(s, 2)

                @pl.when(j + 1 < G)
                def _():
                    xstart(s + 1, 1 - slot)
                xcopy(s, slot).wait()
                yd, xd, cd = dest(s)
                row = tab_in[yd * X + 2 * xd + cd]
                hot = jnp.where(tok == row, 1.0, 0.0).astype(BF16)
                at = pl.ds(pl.multiple_of(j * C, C), C)
                for c0 in range(0, D, NT):
                    r = lax.dot_general(hot, xs[slot, :, c0:c0 + NT], (((0,), (0,)), ((), ())),
                                        preferred_element_type=F32).astype(BF16)
                    for e in range(el):
                        xt[e, at, c0:c0 + NT] = r[e * C:(e + 1) * C]
                return 0

            lax.fori_loop(0, G, pick, 0)

            def odrain(hh):
                for v in range(2):
                    pltpu.make_async_copy(ob.at[hh, :, pl.ds(v * H, H)], stage.at[v, pl.ds(0, half)],
                                          osem.at[hh, v]).wait()

            def ffn(e, _):
                hh = lax.rem(e, 2)

                @pl.when(g == 0)
                def _():
                    for cp in wcopies(e):
                        cp.wait()
                xr = xt[e]
                a = jnp.dot(xr, w1v[e], preferred_element_type=F32)
                b = jnp.dot(xr, w3v[e], preferred_element_type=F32)
                h = (jax.nn.silu(a) * b).astype(BF16)

                @pl.when(e >= 2)
                def _():
                    odrain(hh)
                for c0 in range(0, D, NT):
                    ob[hh, :, c0:c0 + NT] = jnp.dot(h, w2v[e, :, c0:c0 + NT],
                                                    preferred_element_type=F32).astype(BF16)
                for jj in range(G):
                    yd, xd, cd = dest(g * G + jj)
                    at = pl.ds(pl.multiple_of((yd * X + 2 * xd + cd) * B + e * C, C), C)
                    for v in range(2):
                        pltpu.make_async_copy(ob.at[hh, pl.ds(jj * C, C), pl.ds(v * H, H)],
                                              stage.at[v, at], osem.at[hh, v]).start()
                for t, todo in plan.items():
                    @pl.when(g * el + e == t)
                    def _(todo=todo):
                        for h, off in todo:
                            event(h, off)

                @pl.when((e == el - 2) & (g + 1 < NG))
                def _():
                    xstart((g + 1) * G, 0)
                return 0

            lax.fori_loop(0, el, ffn, 0)
            for hh in range(2):
                odrain(hh)

            def go(j, _):
                s = g * G + j
                far_a, far_b = away(s)

                @pl.when(far_a)
                def _():
                    send_a(s).start()

                @pl.when(far_b)
                def _():
                    send_b(s).start()
                return 0

            lax.fori_loop(0, G, go, 0)
            return 0

        lax.fori_loop(0, NG, group, 0)

    def tsend(v, d):
        yo, xo = lax.rem(mo + d, O), lax.rem(mc + d, W)
        if v == 0:
            src, dst, to = pk.at[:, yo], pk_a.at[mo], {'outer': yo, 'expert': mx}
        else:
            src, dst, to = pk.at[:, :, pl.ds(2 * xo, 2)], pk_b.at[mc], {'outer': mo, 'expert': 2 * xo + core}
        return pltpu.make_async_remote_copy(src_ref=src, dst_ref=dst, send_sem=tsem2.at[1 + v, d],
                                            recv_sem=tsem2.at[3 + v, d], device_id=to, device_id_type=MESH)

    pl.run_scoped(experts, pltpu.VMEM((el, D, FF), BF16), pltpu.VMEM((el, D, FF), BF16),
                  pltpu.VMEM((el, FF, D), BF16), pltpu.VMEM((el, half, D), BF16))

    pltpu.make_async_copy(pk.at[:, mo], pk_a.at[mo], tsem2.at[1, 0]).wait()
    pltpu.make_async_copy(pk.at[:, :, pl.ds(2 * mc, 2)], pk_b.at[mc], tsem2.at[2, 0]).wait()
    for d in range(1, 4):
        tsend(0, d).wait()
        tsend(1, d).wait()

    def combine(pa, pb):
        pa[...] = jnp.zeros_like(pa)
        pb[...] = jnp.zeros_like(pb)
        tokf = lax.broadcasted_iota(jnp.int32, (T, 2 * B), 0).astype(F32)

        def origins(p):
            a, b = offs(p)
            return a, b, lax.rem(mo - a + O, O), lax.rem(mc - b + W, W)

        def fetch(p, slot):
            a, b, sy, sx = origins(p)
            yd, xd = lax.rem(mo + a, O), lax.rem(mc + b, W)
            for k in range(2):
                s = 2 * p + k
                c = lax.rem(core + k, 2)
                at = pl.ds(pl.multiple_of(c * B, B), B)
                for v in range(2):
                    if v == 0:
                        src, own = block(recv.at[0], at_a(yd, 2 * sx + c)), block(stage.at[0], yd * X + 2 * mc + core)
                    else:
                        src, own = block(recv.at[1], at_b(xd, sy, c)), block(stage.at[1], mo * X + 2 * xd + core)
                    far = (b if v == 0 else a) > 0

                    def bring(ref, v=v, at=at):
                        pltpu.make_async_copy(ref, xs.at[slot, at, pl.ds(v * H, H)], xsem.at[slot]).start()

                    def take(src=src, v=v, s=s, bring=bring):
                        pltpu.make_async_remote_copy(
                            src_ref=src, dst_ref=src, send_sem=ssem.at[v, s],
                            recv_sem=rsem.at[v, s],
                            device_id={'outer': mo, 'expert': lax.rem(mx + 1, X)},
                            device_id_type=MESH).wait_recv()
                        bring(src)
                    if k == 1:
                        take()
                    else:
                        pl.when(far)(take)
                        pl.when(jnp.logical_not(far))(functools.partial(bring, own))

        def psend(v, d):
            if v == 0:
                src, to = pa.at[d], {'outer': lax.rem(mo + d, O), 'expert': mx}
            else:
                src, to = pb.at[d], {'outer': mo, 'expert': 2 * lax.rem(mc + d, W) + core}
            return pltpu.make_async_remote_copy(
                src_ref=src, dst_ref=part.at[v, d - 1], send_sem=pssem.at[v, d - 1],
                recv_sem=prsem.at[v, d - 1], device_id=to, device_id_type=MESH)

        fetch(0, 0)

        def weights(ref, d, r0):
            out = []
            rows = [ref[(d, 0) + r0(c)] for c in range(2)]
            gs = [ref[(d, 1) + r0(c)] for c in range(2)]
            w = jnp.where(tokf == jnp.concatenate(rows, axis=1), jnp.concatenate(gs, axis=1), 0.0)
            hi = w.astype(BF16)
            r = w - hi.astype(F32)
            mid = r.astype(BF16)
            return hi, mid, (r - mid.astype(F32)).astype(BF16)

        def comb(p, _):
            slot = lax.rem(p, 2)

            @pl.when(p + 1 < n // 2)
            def _():
                fetch(p + 1, 1 - slot)
            a, b, sy, sx = origins(p)
            wa = weights(pk_a, lax.rem(mo + a, O), lambda c: (2 * sx + c,))
            wb = weights(pk_b, lax.rem(mc + b, W), lambda c: (sy, c))
            pltpu.make_async_copy(xall.at[pl.ds(0, T)], xs.at[slot], xsem.at[slot]).wait()
            for acc, d, ws, base in ((pa, a, wa, 0), (pb, b, wb, H)):
                for c0 in range(0, H, NT):
                    rr = xs[slot, :, base + c0:base + c0 + NT]
                    acc[d, :, c0:c0 + NT] += (jnp.dot(ws[0], rr, preferred_element_type=F32)
                                              + jnp.dot(ws[1], rr, preferred_element_type=F32)
                                              + jnp.dot(ws[2], rr, preferred_element_type=F32))
            for last, v, ds in ((11, 0, (1, 3)), (13, 1, (1, 3)), (15, 0, (2,)), (15, 1, (2,))):
                @pl.when(p == last)
                def _(v=v, ds=ds):
                    for d in ds:
                        psend(v, d).start()
            return 0

        lax.fori_loop(0, n // 2, comb, 0)

        def sent(s, _):
            far_a, far_b = away(s)

            @pl.when(far_a)
            def _():
                send_a(s).wait_send()

            @pl.when(far_b)
            def _():
                send_b(s).wait_send()
            return 0

        lax.fori_loop(0, n, sent, 0)

        def wsend(ref, sem):
            pltpu.make_async_remote_copy(src_ref=ref, dst_ref=ref, send_sem=sem, recv_sem=tsem.at[1],
                                         device_id=other(), device_id_type=MESH).wait_send()

        def gone(i, _):
            wsend(xall.at[pl.ds(0, T // 2)], gsem.at[i])
            return 0

        lax.fori_loop(0, len(FULL), gone, 0)

        def gonep(i, _):
            wsend(xall.at[pl.ds(0, T // 4)], gpsem.at[i])
            return 0

        lax.fori_loop(0, len(PIECE), gonep, 0)

        def goneh(i, _):
            wsend(xall.at[pl.ds(0, T // 2)], hsem.at[i])
            return 0

        lax.fori_loop(0, n, goneh, 0)
        wsend(tab_in.at[pl.ds(0, n - 1)], tsem.at[0])

        accs = (pa, pb)
        for d in (1, 3, 2):
            for v in range(2):
                psend(v, d).wait()
                pltpu.make_async_copy(part.at[v, d - 1], accs[v].at[d], prsem.at[v, d - 1]).start()
            for v in range(2):
                pltpu.make_async_copy(part.at[v, d - 1], accs[v].at[d], prsem.at[v, d - 1]).wait()
                if d != 2:
                    accs[v][0] += accs[v][d]
        for v in range(2):
            for hh in range(T // half):
                rows = slice(hh * half, (hh + 1) * half)
                ob[hh, :, v * H:(v + 1) * H] = (accs[v][0, rows] + accs[v][2, rows]).astype(BF16)
        cps = [pltpu.make_async_copy(ob.at[hh], y.at[pl.ds(hh * half, half)], osem.at[hh, 0])
               for hh in range(T // half)]
        for cp in cps:
            cp.start()
        for cp in cps:
            cp.wait()

    pl.run_scoped(combine, pltpu.VMEM((O, T, H), F32), pltpu.VMEM((W, T, H), F32))


def solution(mesh):
    O = mesh.shape['outer']
    X = mesh.shape['expert']
    n = O * X
    tok = P(('data', 'outer', 'expert'), None)
    wsp = P(('outer', 'expert'), None, None)

    def local(x, wr, idx, w1, w3, w2):
        T, D = x.shape
        k = idx.shape[1]
        E = wr.shape[1]
        el, _, FF = w1.shape
        C = 2 * T * k // E
        B = el * C
        g = _gate(x, wr, idx)
        tab, gs = _tables(idx, g, E, C)
        pk = jnp.stack((tab.astype(F32), gs)).reshape(2, O, X, 1, B)
        anyspec = pl.BlockSpec(memory_space=pl.ANY)
        y = pl.pallas_call(
            functools.partial(_kernel, O, X, el, C),
            out_shape=(jax.ShapeDtypeStruct((T, D), BF16),
                       jax.ShapeDtypeStruct((n * T, D), BF16),
                       jax.ShapeDtypeStruct((2, n * B, D // 2), BF16),
                       jax.ShapeDtypeStruct((2, n * B, D // 2), BF16),
                       jax.ShapeDtypeStruct((2, O - 1, T, D // 2), F32)),
            in_specs=[anyspec] * 5,
            out_specs=(anyspec,) * 5,
            scratch_shapes=[
                pltpu.VMEM((2, T, D), BF16),
                pltpu.VMEM((2, 4 * C, D), BF16),
                pltpu.VMEM((n, 1, B), F32),
                pltpu.VMEM((O, 2, X, 1, B), F32),
                pltpu.VMEM((X // 2, 2, O, 2, 1, B), F32),
                pltpu.SemaphoreType.DMA((3, el)),
                pltpu.SemaphoreType.DMA((2,)),
                pltpu.SemaphoreType.DMA((2, 2)),
                pltpu.SemaphoreType.DMA((2, n)),
                pltpu.SemaphoreType.DMA((2, n)),
                pltpu.SemaphoreType.DMA((2, O - 1)),
                pltpu.SemaphoreType.DMA((2, O - 1)),
                pltpu.SemaphoreType.DMA((32,)),
                pltpu.SemaphoreType.DMA((64,)),
                pltpu.SemaphoreType.DMA((32,)),
                pltpu.SemaphoreType.DMA((32,)),
                pltpu.SemaphoreType.DMA((16,)),
                pltpu.SemaphoreType.DMA((32,)),
                pltpu.SemaphoreType.DMA((2,)),
                pltpu.SemaphoreType.DMA((5, 4)),
            ],
            compiler_params=pltpu.CompilerParams(
                collective_id=0, has_side_effects=True, vmem_limit_bytes=67043328),
        )(x, pk, w1, w3, w2)
        return y[0]

    return jax.shard_map(local, mesh=mesh, in_specs=(tok, P(None, None), tok, wsp, wsp, wsp), out_specs=tok, check_vma=False)
```

```python
import functools

import jax
import jax.numpy as jnp
from jax import lax
from jax.experimental import pallas as pl
from jax.experimental.pallas import tpu as pltpu
from jax.sharding import PartitionSpec as P

MESH = pl.DeviceIdType.MESH
F32 = jnp.float32
BF16 = jnp.bfloat16


def _gate(x, wr, idx):
    logits = jnp.dot(x, wr, preferred_element_type=F32)
    oh = idx[:, :, None] == jnp.arange(wr.shape[1], dtype=idx.dtype)
    return jax.nn.softmax(jnp.sum(jnp.where(oh, logits[:, None, :], 0.0), axis=-1), axis=-1)


def _parts(w):
    hi = lax.reduce_precision(w, 8, 7)
    r = w - hi
    mid = lax.reduce_precision(r, 8, 7)
    return hi, mid, r - mid


def _tables(idx, g, E, C):
    t, k = idx.shape
    oh = idx[:, :, None] == jnp.arange(E, dtype=idx.dtype)
    m = jnp.sum(oh, axis=1, dtype=jnp.int32).astype(BF16)
    pos = jnp.arange(t, dtype=jnp.int32)
    tri = (pos[None, :] < pos[:, None]).astype(BF16)
    cnt = jnp.dot(tri, m, preferred_element_type=F32)
    r = jnp.sum(jnp.where(oh, cnt[:, None, :], 0.0), axis=-1)
    ohr = r[:, :, None] == jnp.arange(C, dtype=F32)
    one = jnp.ones((t, k), F32)
    lo = (pos % 256).astype(F32)[:, None] * one
    hi = (pos // 256).astype(F32)[:, None] * one
    vals = jnp.stack((one, hi, lo) + _parts(g), axis=-1)
    rhs = jnp.where(ohr[:, :, None, :], vals[..., None], 0.0).astype(BF16)
    res = jnp.einsum('tje,tjic->iec', oh.astype(BF16), rhs, preferred_element_type=F32)
    tab = jnp.where(res[0] > 0.5, res[1] * 256.0 + res[2], -1.0).astype(jnp.int32)
    return tab, (res[3] + res[4]) + res[5]


ORDER = ((0, 1), (0, 3), (1, 0), (3, 0), (0, 0), (0, 2), (1, 1), (3, 3),
         (1, 3), (3, 1), (1, 2), (3, 2), (2, 1), (2, 3), (2, 0), (2, 2))
NEAR = (1, 3)
EARLY, MID, LATE = range(3)
HERE = (0, 0)
TIMES = (0, 3, 5, 6, 8, 9, 12, 13, 15, 16, 20)


def _lut(vals, i):
    r = vals[0]
    for k in range(1, len(vals)):
        r = jnp.where(i == k, vals[k], r)
    return r


def _relays(h, off):
    u, v = off
    if v == 0:
        if u == 3:
            return ((0, 1, 0), (1, 1, None), (1, 3, None))
        if u == 1:
            return ((0, 3, 1), (1, 1, None), (1, 3, None))
        return ((1, 1, None), (1, 3, None))
    if v == 3:
        return ((1, 1, 0),)
    if v == 1:
        return ((1, 3, 1),)
    return ()


def _numbered():
    full, piece = {}, {}
    for h in range(2):
        for d in NEAR:
            for axis in range(2):
                full[(h, HERE, axis, d)] = len(full)
        for off in ORDER:
            if off != HERE:
                for axis, d, part in _relays(h, off):
                    table = full if part is None else piece
                    table[(h, off, axis, d)] = len(table)
    return full, piece


FULL, PIECE = _numbered()


def _kernel(O, X, el, C, x, pk, w1, w3, w2, y, xall, stage, recv, part,
            xs, ob, tab_in, pk_a, pk_b, mid, wsem, xsem, osem, ssem, rsem, pssem, prsem, psem,
            bsem, bpsem, gsem, gpsem, dsem, hsem, tsem, tsem2):
    n = O * X
    W = X // 2
    _, T, D = xs.shape
    H = D // 2
    FF = w1.shape[2]
    B = el * C
    G = 4
    NG = n // G
    half = G * C
    NT = 512
    mo = lax.axis_index('outer')
    mx = lax.axis_index('expert')
    mc = mx // 2
    core = lax.rem(mx, 2)
    me = mo * X + mx

    def offs(p):
        return _lut([o[0] for o in ORDER], p), _lut([o[1] for o in ORDER], p)

    def dest(s):
        a, b = offs(s // 2)
        return lax.rem(mo + a, O), lax.rem(mc + b, W), lax.rem(core + lax.rem(s, 2), 2)

    def block(ref, d):
        return ref.at[pl.ds(pl.multiple_of(d * B, B), B)]

    def at_a(yd, sx):
        return yd * X + sx

    def at_b(xd, sy, sc):
        return xd * X + sy * 2 + sc

    bar = pltpu.get_barrier_semaphore()

    def greet(d, _):
        t = lax.rem(me + d, n)
        pl.semaphore_signal(bar, inc=1, device_id={'outer': t // X, 'expert': lax.rem(t, X)}, device_id_type=MESH)
        return 0

    lax.fori_loop(1, n, greet, 0)

    def rows(ref, a, b, h, piece, c=None):
        src = lax.rem(mo + a, O) * X + 2 * lax.rem(mc + b, W) + (core if c is None else c)
        step = T // 2
        if piece is None:
            return ref.at[pl.ds(pl.multiple_of(src * T + h * step, step), step)]
        return ref.at[pl.ds(pl.multiple_of(src * T + h * step + piece * (step // 2), step // 2), step // 2)]

    def neighbour(h, axis, d):
        if (axis == 0) == (h == 0):
            return {'outer': mo, 'expert': 2 * lax.rem(mc + d, W) + core}
        return {'outer': lax.rem(mo + d, O), 'expert': mx}

    def offset(h, off):
        return (off[1], off[0]) if h == 0 else off

    def relay(h, off, axis, d, piece, src=None):
        a, b = offset(h, off)
        key = (h, off, axis, d)
        send = gsem.at[FULL[key]] if piece is None else gpsem.at[PIECE[key]]
        u, v = off
        seen = ((u - d) % 4, v) if axis == 0 else (u, (v - d) % 4)
        ra, rb = offset(h, seen)
        k = h * 16 + ra * 4 + rb
        recv_ = bsem.at[k] if piece is None else bpsem.at[2 * k + piece]
        dst = rows(xall, a, b, h, piece)
        pltpu.make_async_remote_copy(src_ref=dst if src is None else src, dst_ref=dst, send_sem=send, recv_sem=recv_,
                                     device_id=neighbour(h, axis, d), device_id_type=MESH).start()

    def share(h, off, src=None):
        a, b = offset(h, off)
        dst = rows(xall, a, b, h, None)
        pltpu.make_async_remote_copy(
            src_ref=dst if src is None else src, dst_ref=dst, send_sem=hsem.at[h * 16 + a * 4 + b],
            recv_sem=dsem.at[a * 4 + b], device_id={'outer': mo, 'expert': 2 * mc + 1 - core},
            device_id_type=MESH).start()

    def other():
        return {'outer': mo, 'expert': 2 * mc + 1 - core}

    def arrive(ref, sem):
        pltpu.make_async_remote_copy(src_ref=ref, dst_ref=ref, send_sem=hsem.at[0], recv_sem=sem,
                                     device_id=other(), device_id_type=MESH).wait_recv()

    def event(h, off):
        a, b = offset(h, off)
        k = h * 16 + a * 4 + b
        if off[1] == 2 or off == (2, 0):
            for piece in range(2):
                arrive(rows(xall, a, b, h, piece), bpsem.at[2 * k + piece])
        else:
            arrive(rows(xall, a, b, h, None), bsem.at[k])
        for axis, d, piece in _relays(h, off):
            relay(h, off, axis, d, piece)
        share(h, off)

    def xcopy(s, slot):
        yd, xd, cd = dest(s)
        at = pl.ds(pl.multiple_of((yd * X + 2 * xd + cd) * T, T), T)
        return pltpu.make_async_copy(xall.at[at], xs.at[slot], xsem.at[slot])

    def xstart(s, slot):
        a, b = offs(s // 2)
        kk = lax.rem(s, 2)
        mine = (a + b + kk) == 0

        @pl.when(kk == 1)
        def _():
            yd, xd, cd = dest(s)
            at = pl.ds(pl.multiple_of((yd * X + 2 * xd + cd) * T, T), T)
            arrive(xall.at[at], dsem.at[a * 4 + b])

        @pl.when(mine)
        def _():
            pltpu.make_async_copy(x, xs.at[slot], xsem.at[slot]).start()

        @pl.when(jnp.logical_not(mine))
        def _():
            xcopy(s, slot).start()

    def send_a(s):
        yd, xd, cd = dest(s)
        return pltpu.make_async_remote_copy(
            src_ref=block(stage.at[0], yd * X + 2 * xd + cd), dst_ref=block(recv.at[0], at_a(yd, mx)),
            send_sem=ssem.at[0, s], recv_sem=rsem.at[0, s],
            device_id={'outer': mo, 'expert': 2 * xd + cd}, device_id_type=MESH)

    def send_b(s):
        yd, xd, cd = dest(s)
        return pltpu.make_async_remote_copy(
            src_ref=block(stage.at[1], yd * X + 2 * xd + cd), dst_ref=block(recv.at[1], at_b(xd, mo, core)),
            send_sem=ssem.at[1, s], recv_sem=rsem.at[1, s],
            device_id={'outer': yd, 'expert': 2 * mc + cd}, device_id_type=MESH)

    def away(s):
        a, b = offs(s // 2)
        k = lax.rem(s, 2)
        return b + k > 0, a + k > 0

    def experts(w1v, w3v, w2v, xt):
        def wcopies(e):
            return (pltpu.make_async_copy(w1.at[e], w1v.at[e], wsem.at[0, e]),
                    pltpu.make_async_copy(w3.at[e], w3v.at[e], wsem.at[1, e]),
                    pltpu.make_async_copy(w2.at[e], w2v.at[e], wsem.at[2, e]))

        pl.semaphore_wait(bar, n - 1)
        step = T // 2
        own = [x.at[pl.ds(h * step, step)] for h in range(2)]
        for axis in range(2):
            for h in range(2):
                for d in NEAR:
                    relay(h, HERE, axis, d, None, own[h])
        for h in range(2):
            share(h, HERE, own[h])

        def tell(d, _):
            t = lax.rem(me + d, n)
            to, tx = t // X, lax.rem(t, X)
            pltpu.make_async_remote_copy(
                src_ref=pk.at[0, to, tx], dst_ref=tab_in.at[me], send_sem=tsem.at[0], recv_sem=tsem.at[1],
                device_id={'outer': to, 'expert': tx}, device_id_type=MESH).start()
            return 0

        lax.fori_loop(1, n, tell, 0)
        pltpu.make_async_copy(pk.at[0, mo, mx], tab_in.at[me], tsem2.at[0, 0]).start()
        for d in range(4):
            yo, xo = lax.rem(mo + d, O), lax.rem(mc + d, W)
            if d == 0:
                pltpu.make_async_copy(pk.at[:, mo], pk_a.at[mo], tsem2.at[1, 0]).start()
                pltpu.make_async_copy(pk.at[:, :, pl.ds(2 * mc, 2)], pk_b.at[mc], tsem2.at[2, 0]).start()
            else:
                tsend(0, d).start()
                tsend(1, d).start()
        for e in range(el):
            for cp in wcopies(e):
                cp.start()
        tok = lax.broadcasted_iota(jnp.int32, (T, B), 0).astype(F32)

        for axis in range(2):
            for h in range(2):
                for d in NEAR:
                    event(h, (0, d) if axis else (d, 0))
        pltpu.make_async_copy(pk.at[0, mo, mx], tab_in.at[me], tsem2.at[0, 0]).wait()
        allrows = pltpu.make_async_remote_copy(
            src_ref=tab_in.at[pl.ds(0, n - 1)], dst_ref=tab_in.at[pl.ds(0, n - 1)], send_sem=tsem.at[0],
            recv_sem=tsem.at[1], device_id=other(), device_id_type=MESH)
        allrows.wait_recv()

        later = [(2, 0), (0, 2)] + [(u, v) for u in NEAR for v in NEAR]
        later += [(2, v) for v in NEAR] + [(u, 2) for u in NEAR] + [(2, 2)]
        plan = dict(zip(TIMES, later))

        xstart(0, 0)

        def group(g, _):
            def pick(j, _):
                s = g * G + j
                slot = lax.rem(s, 2)

                @pl.when(j + 1 < G)
                def _():
                    xstart(s + 1, 1 - slot)
                xcopy(s, slot).wait()
                yd, xd, cd = dest(s)
                row = tab_in[yd * X + 2 * xd + cd]
                hot = jnp.where(tok == row, 1.0, 0.0).astype(BF16)
                at = pl.ds(pl.multiple_of(j * C, C), C)
                for c0 in range(0, D, NT):
                    r = lax.dot_general(hot, xs[slot, :, c0:c0 + NT], (((0,), (0,)), ((), ())),
                                        preferred_element_type=F32).astype(BF16)
                    for e in range(el):
                        xt[e, at, c0:c0 + NT] = r[e * C:(e + 1) * C]
                return 0

            lax.fori_loop(0, G, pick, 0)

            def odrain(hh):
                for v in range(2):
                    pltpu.make_async_copy(ob.at[hh, :, pl.ds(v * H, H)], stage.at[v, pl.ds(0, half)],
                                          osem.at[hh, v]).wait()

            def ffn(e, _):
                hh = lax.rem(e, 2)

                @pl.when(g == 0)
                def _():
                    for cp in wcopies(e):
                        cp.wait()
                xr = xt[e]
                a = jnp.dot(xr, w1v[e], preferred_element_type=F32)
                b = jnp.dot(xr, w3v[e], preferred_element_type=F32)
                h = (jax.nn.silu(a) * b).astype(BF16)

                @pl.when(e >= 2)
                def _():
                    odrain(hh)
                for c0 in range(0, D, NT):
                    ob[hh, :, c0:c0 + NT] = jnp.dot(h, w2v[e, :, c0:c0 + NT],
                                                    preferred_element_type=F32).astype(BF16)
                for jj in range(G):
                    yd, xd, cd = dest(g * G + jj)
                    at = pl.ds(pl.multiple_of((yd * X + 2 * xd + cd) * B + e * C, C), C)
                    for v in range(2):
                        pltpu.make_async_copy(ob.at[hh, pl.ds(jj * C, C), pl.ds(v * H, H)],
                                              stage.at[v, at], osem.at[hh, v]).start()
                for t, todo in plan.items():
                    @pl.when(g * el + e == t)
                    def _(todo=todo):
                        for h in range(2):
                            event(h, todo)

                @pl.when((e == el - 2) & (g + 1 < NG))
                def _():
                    xstart((g + 1) * G, 0)
                return 0

            lax.fori_loop(0, el, ffn, 0)
            for hh in range(2):
                odrain(hh)

            def go(j, _):
                s = g * G + j
                far_a, far_b = away(s)

                @pl.when(far_a)
                def _():
                    send_a(s).start()

                @pl.when(far_b)
                def _():
                    send_b(s).start()
                return 0

            lax.fori_loop(0, G, go, 0)
            return 0

        lax.fori_loop(0, NG, group, 0)

    def tsend(v, d):
        yo, xo = lax.rem(mo + d, O), lax.rem(mc + d, W)
        if v == 0:
            src, dst, to = pk.at[:, yo], pk_a.at[mo], {'outer': yo, 'expert': mx}
        else:
            src, dst, to = pk.at[:, :, pl.ds(2 * xo, 2)], pk_b.at[mc], {'outer': mo, 'expert': 2 * xo + core}
        return pltpu.make_async_remote_copy(src_ref=src, dst_ref=dst, send_sem=tsem2.at[1 + v, d],
                                            recv_sem=tsem2.at[3 + v, d], device_id=to, device_id_type=MESH)

    pl.run_scoped(experts, pltpu.VMEM((el, D, FF), BF16), pltpu.VMEM((el, D, FF), BF16),
                  pltpu.VMEM((el, FF, D), BF16), pltpu.VMEM((el, half, D), BF16))

    pltpu.make_async_copy(pk.at[:, mo], pk_a.at[mo], tsem2.at[1, 0]).wait()
    pltpu.make_async_copy(pk.at[:, :, pl.ds(2 * mc, 2)], pk_b.at[mc], tsem2.at[2, 0]).wait()
    for d in range(1, 4):
        tsend(0, d).wait()
        tsend(1, d).wait()

    def combine(pa, pb):
        pa[...] = jnp.zeros_like(pa)
        pb[...] = jnp.zeros_like(pb)
        tokf = lax.broadcasted_iota(jnp.int32, (T, 2 * B), 0).astype(F32)

        def origins(p):
            a, b = offs(p)
            return a, b, lax.rem(mo - a + O, O), lax.rem(mc - b + W, W)

        def fetch(p, slot):
            a, b, sy, sx = origins(p)
            yd, xd = lax.rem(mo + a, O), lax.rem(mc + b, W)
            for k in range(2):
                s = 2 * p + k
                c = lax.rem(core + k, 2)
                at = pl.ds(pl.multiple_of(c * B, B), B)
                for v in range(2):
                    if v == 0:
                        src, own = block(recv.at[0], at_a(yd, 2 * sx + c)), block(stage.at[0], yd * X + 2 * mc + core)
                    else:
                        src, own = block(recv.at[1], at_b(xd, sy, c)), block(stage.at[1], mo * X + 2 * xd + core)
                    far = (b if v == 0 else a) > 0

                    def bring(ref, v=v, at=at):
                        pltpu.make_async_copy(ref, xs.at[slot, at, pl.ds(v * H, H)], xsem.at[slot]).start()

                    def take(src=src, v=v, s=s, bring=bring):
                        pltpu.make_async_remote_copy(
                            src_ref=src, dst_ref=src, send_sem=ssem.at[v, s],
                            recv_sem=rsem.at[v, s],
                            device_id={'outer': mo, 'expert': lax.rem(mx + 1, X)},
                            device_id_type=MESH).wait_recv()
                        bring(src)
                    if k == 1:
                        take()
                    else:
                        pl.when(far)(take)
                        pl.when(jnp.logical_not(far))(functools.partial(bring, own))

        accs = (pa, pb)
        hr = T // 2
        pairs = [(v, r) for v in range(2) for r in range(2)]

        def late(r):
            return pl.ds(r * hr, hr)

        def psend(kind, v, r):
            d = NEAR[r]
            if kind == EARLY:
                src, dst = accs[v].at[d, late(1 - r)], part.at[v, r, late(1 - r)]
            elif kind == MID:
                src, dst = accs[v].at[2, late(r)], mid.at[v, r]
            else:
                src, dst = accs[v].at[d, late(r)], part.at[v, r, late(r)]
            if v == 0:
                to = {'outer': lax.rem(mo + d, O), 'expert': mx}
            else:
                to = {'outer': mo, 'expert': 2 * lax.rem(mc + d, W) + core}
            return pltpu.make_async_remote_copy(
                src_ref=src, dst_ref=dst, send_sem=pssem.at[kind, v, r], recv_sem=prsem.at[kind, v, r],
                device_id=to, device_id_type=MESH)

        fetch(0, 0)

        def weights(ref, d, r0):
            rows = [ref[(d, 0) + r0(c)] for c in range(2)]
            gs = [ref[(d, 1) + r0(c)] for c in range(2)]
            w = jnp.where(tokf == jnp.concatenate(rows, axis=1), jnp.concatenate(gs, axis=1), 0.0)
            hi = w.astype(BF16)
            r = w - hi.astype(F32)
            mid = r.astype(BF16)
            return hi, mid, (r - mid.astype(F32)).astype(BF16)

        def comb(p, _):
            slot = lax.rem(p, 2)

            @pl.when(p + 1 < n // 2)
            def _():
                fetch(p + 1, 1 - slot)
            a, b, sy, sx = origins(p)
            wa = weights(pk_a, lax.rem(mo + a, O), lambda c: (2 * sx + c,))
            wb = weights(pk_b, lax.rem(mc + b, W), lambda c: (sy, c))
            pltpu.make_async_copy(xall.at[pl.ds(0, T)], xs.at[slot], xsem.at[slot]).wait()
            for acc, d, ws, base in ((pa, a, wa, 0), (pb, b, wb, H)):
                for c0 in range(0, H, NT):
                    rr = xs[slot, :, base + c0:base + c0 + NT]
                    acc[d, :, c0:c0 + NT] += (jnp.dot(ws[0], rr, preferred_element_type=F32)
                                              + jnp.dot(ws[1], rr, preferred_element_type=F32)
                                              + jnp.dot(ws[2], rr, preferred_element_type=F32))
            for last, kind, sides in ((11, EARLY, pairs[:2]), (13, EARLY, pairs[2:]), (15, MID, pairs)):
                @pl.when(p == last)
                def _(kind=kind, sides=sides):
                    for v, r in sides:
                        psend(kind, v, r).start()
            return 0

        lax.fori_loop(0, n // 2, comb, 0)

        def land(v, r, half_):
            return pltpu.make_async_copy(part.at[v, r, late(half_)], accs[v].at[NEAR[r], late(half_)], psem.at[v, r])

        for v, r in pairs:
            psend(EARLY, v, r).wait()
            land(v, r, 1 - r).start()
        for v, r in pairs:
            land(v, r, 1 - r).wait()
            accs[v][0, late(1 - r)] += accs[v][NEAR[r], late(1 - r)]
        for v, r in pairs:
            psend(MID, v, r).wait()
            accs[v][NEAR[r], late(r)] += mid[v, r]
            psend(LATE, v, r).start()

        def sent(s, _):
            far_a, far_b = away(s)

            @pl.when(far_a)
            def _():
                send_a(s).wait_send()

            @pl.when(far_b)
            def _():
                send_b(s).wait_send()
            return 0

        lax.fori_loop(0, n, sent, 0)

        def wsend(ref, sem):
            pltpu.make_async_remote_copy(src_ref=ref, dst_ref=ref, send_sem=sem, recv_sem=tsem.at[1],
                                         device_id=other(), device_id_type=MESH).wait_send()

        def gone(i, _):
            wsend(xall.at[pl.ds(0, T // 2)], gsem.at[i])
            return 0

        lax.fori_loop(0, len(FULL), gone, 0)

        def gonep(i, _):
            wsend(xall.at[pl.ds(0, T // 4)], gpsem.at[i])
            return 0

        lax.fori_loop(0, len(PIECE), gonep, 0)

        def goneh(i, _):
            wsend(xall.at[pl.ds(0, T // 2)], hsem.at[i])
            return 0

        lax.fori_loop(0, n, goneh, 0)
        wsend(tab_in.at[pl.ds(0, n - 1)], tsem.at[0])

        for v, r in pairs:
            psend(LATE, v, r).wait()
            land(v, r, r).start()
        for v, r in pairs:
            land(v, r, r).wait()
            ob[r, :, v * H:(v + 1) * H] = (accs[v][0, late(r)] + accs[v][NEAR[r], late(r)]).astype(BF16)
        cps = [pltpu.make_async_copy(ob.at[hh], y.at[pl.ds(hh * half, half)], osem.at[hh, 0])
               for hh in range(T // half)]
        for cp in cps:
            cp.start()
        for cp in cps:
            cp.wait()

    pl.run_scoped(combine, pltpu.VMEM((O, T, H), F32), pltpu.VMEM((W, T, H), F32))


def solution(mesh):
    O = mesh.shape['outer']
    X = mesh.shape['expert']
    n = O * X
    tok = P(('data', 'outer', 'expert'), None)
    wsp = P(('outer', 'expert'), None, None)

    def local(x, wr, idx, w1, w3, w2):
        T, D = x.shape
        k = idx.shape[1]
        E = wr.shape[1]
        el, _, FF = w1.shape
        C = 2 * T * k // E
        B = el * C
        g = _gate(x, wr, idx)
        tab, gs = _tables(idx, g, E, C)
        pk = jnp.stack((tab.astype(F32), gs)).reshape(2, O, X, 1, B)
        anyspec = pl.BlockSpec(memory_space=pl.ANY)
        y = pl.pallas_call(
            functools.partial(_kernel, O, X, el, C),
            out_shape=(jax.ShapeDtypeStruct((T, D), BF16),
                       jax.ShapeDtypeStruct((n * T, D), BF16),
                       jax.ShapeDtypeStruct((2, n * B, D // 2), BF16),
                       jax.ShapeDtypeStruct((2, n * B, D // 2), BF16),
                       jax.ShapeDtypeStruct((2, 2, T, D // 2), F32)),
            in_specs=[anyspec] * 5,
            out_specs=(anyspec,) * 5,
            scratch_shapes=[
                pltpu.VMEM((2, T, D), BF16),
                pltpu.VMEM((2, 4 * C, D), BF16),
                pltpu.VMEM((n, 1, B), F32),
                pltpu.VMEM((O, 2, X, 1, B), F32),
                pltpu.VMEM((X // 2, 2, O, 2, 1, B), F32),
                pltpu.VMEM((2, 2, T // 2, D // 2), F32),
                pltpu.SemaphoreType.DMA((3, el)),
                pltpu.SemaphoreType.DMA((2,)),
                pltpu.SemaphoreType.DMA((2, 2)),
                pltpu.SemaphoreType.DMA((2, n)),
                pltpu.SemaphoreType.DMA((2, n)),
                pltpu.SemaphoreType.DMA((3, 2, 2)),
                pltpu.SemaphoreType.DMA((3, 2, 2)),
                pltpu.SemaphoreType.DMA((2, 2)),
                pltpu.SemaphoreType.DMA((32,)),
                pltpu.SemaphoreType.DMA((64,)),
                pltpu.SemaphoreType.DMA((32,)),
                pltpu.SemaphoreType.DMA((32,)),
                pltpu.SemaphoreType.DMA((16,)),
                pltpu.SemaphoreType.DMA((32,)),
                pltpu.SemaphoreType.DMA((2,)),
                pltpu.SemaphoreType.DMA((5, 4)),
            ],
            compiler_params=pltpu.CompilerParams(
                collective_id=0, has_side_effects=True, vmem_limit_bytes=67043328),
        )(x, pk, w1, w3, w2)
        return y[0]

    return jax.shard_map(local, mesh=mesh, in_specs=(tok, P(None, None), tok, wsp, wsp, wsp), out_specs=tok, check_vma=False)
```

```python
import functools

import jax
import jax.numpy as jnp
from jax import lax
from jax.experimental import pallas as pl
from jax.experimental.pallas import tpu as pltpu
from jax.sharding import PartitionSpec as P

MESH = pl.DeviceIdType.MESH
F32 = jnp.float32
BF16 = jnp.bfloat16


def _split(w):
    hi = w.astype(BF16)
    r = w - hi.astype(F32)
    mid = r.astype(BF16)
    return hi, mid, (r - mid.astype(F32)).astype(BF16)


def _tables(xv, wr, idx, C):
    T, k = idx.shape
    E = wr.shape[1]
    logits = jnp.dot(xv, wr, preferred_element_type=F32)
    lane = lax.broadcasted_iota(jnp.int32, (T, E), 1)
    hits = [idx[:, j:j + 1] == lane for j in range(k)]

    def take(table):
        return [jnp.sum(jnp.where(h, table, 0.0), axis=1, keepdims=True) for h in hits]

    at = take(logits)
    top = functools.reduce(jnp.maximum, at)
    ex = [jnp.exp(v - top) for v in at]
    tot = functools.reduce(jnp.add, ex)
    ones = [jnp.where(h, 1.0, 0.0) for h in hits]
    many = functools.reduce(jnp.add, ones).astype(BF16)
    tri = lax.broadcasted_iota(jnp.int32, (T, T), 1) < lax.broadcasted_iota(jnp.int32, (T, T), 0)
    rank = take(jnp.dot(jnp.where(tri, 1.0, 0.0).astype(BF16), many, preferred_element_type=F32))
    slot = lax.rem(lane, C).astype(F32)
    left = lane < C
    tok = lax.broadcasted_iota(jnp.int32, (T, 1), 0) + 1
    lo = lax.rem(tok, T // 2).astype(F32)
    hi = (tok // (T // 2)).astype(F32)
    res = [0.0] * 3
    for j in range(k):
        g = [v.astype(F32) for v in _split(ex[j] / tot)]
        hot = ones[j].astype(BF16)
        here = rank[j] == slot
        for i, (u, v) in enumerate(((hi, lo), (g[0], g[1]), (g[2], g[2]))):
            val = jnp.where(here, jnp.where(left, u, v), 0.0).astype(BF16)
            res[i] += lax.dot_general(hot, val, (((0,), (0,)), ((), ())), preferred_element_type=F32)
    tab = res[0][:, :C] * (T // 2) + res[0][:, C:2 * C] - 1.0
    return tab, (res[1][:, :C] + res[1][:, C:2 * C]) + res[2][:, :C]


ORDER = ((0, 1), (0, 3), (1, 0), (3, 0), (0, 0), (0, 2), (1, 1), (3, 3),
         (1, 3), (3, 1), (1, 2), (3, 2), (2, 1), (2, 3), (2, 0), (2, 2))
NEAR = (1, 3)
EARLY, MID, LATE = range(3)
HERE = (0, 0)
TIMES = (0, 3, 5, 6, 8, 9, 12, 13, 15, 16, 20)


def _lut(vals, i):
    r = vals[0]
    for k in range(1, len(vals)):
        r = jnp.where(i == k, vals[k], r)
    return r


def _relays(h, off):
    u, v = off
    if v == 0:
        if u == 3:
            return ((0, 1, 0), (1, 1, None), (1, 3, None))
        if u == 1:
            return ((0, 3, 1), (1, 1, None), (1, 3, None))
        return ((1, 1, None), (1, 3, None))
    if v == 3:
        return ((1, 1, 0),)
    if v == 1:
        return ((1, 3, 1),)
    return ()


def _numbered():
    full, piece = {}, {}
    for h in range(2):
        for d in NEAR:
            for axis in range(2):
                full[(h, HERE, axis, d)] = len(full)
        for off in ORDER:
            if off != HERE:
                for axis, d, part in _relays(h, off):
                    table = full if part is None else piece
                    table[(h, off, axis, d)] = len(table)
    return full, piece


FULL, PIECE = _numbered()


def _kernel(O, X, el, C, x, wr, idx, w1, w3, w2, y, xall, stage, recv, part,
            xs, ob, pk, flat, tab_in, pk_a, pk_b, mid, wsem, xsem, osem, ssem, rsem, pssem, prsem, psem,
            bsem, bpsem, gsem, gpsem, dsem, hsem, tsem, tsem2):
    n = O * X
    W = X // 2
    _, T, D = xs.shape
    H = D // 2
    FF = w1.shape[2]
    B = el * C
    G = 4
    NG = n // G
    half = G * C
    NT = 512
    mo = lax.axis_index('outer')
    mx = lax.axis_index('expert')
    mc = mx // 2
    core = lax.rem(mx, 2)
    me = mo * X + mx

    def offs(p):
        return _lut([o[0] for o in ORDER], p), _lut([o[1] for o in ORDER], p)

    def dest(s):
        a, b = offs(s // 2)
        return lax.rem(mo + a, O), lax.rem(mc + b, W), lax.rem(core + lax.rem(s, 2), 2)

    def block(ref, d):
        return ref.at[pl.ds(pl.multiple_of(d * B, B), B)]

    def at_a(yd, sx):
        return yd * X + sx

    def at_b(xd, sy, sc):
        return xd * X + sy * 2 + sc

    bar = pltpu.get_barrier_semaphore()

    def greet(d, _):
        t = lax.rem(me + d, n)
        pl.semaphore_signal(bar, inc=1, device_id={'outer': t // X, 'expert': lax.rem(t, X)}, device_id_type=MESH)
        return 0

    lax.fori_loop(1, n, greet, 0)

    def rows(ref, a, b, h, piece, c=None):
        src = lax.rem(mo + a, O) * X + 2 * lax.rem(mc + b, W) + (core if c is None else c)
        step = T // 2
        if piece is None:
            return ref.at[pl.ds(pl.multiple_of(src * T + h * step, step), step)]
        return ref.at[pl.ds(pl.multiple_of(src * T + h * step + piece * (step // 2), step // 2), step // 2)]

    def neighbour(h, axis, d):
        if (axis == 0) == (h == 0):
            return {'outer': mo, 'expert': 2 * lax.rem(mc + d, W) + core}
        return {'outer': lax.rem(mo + d, O), 'expert': mx}

    def offset(h, off):
        return (off[1], off[0]) if h == 0 else off

    def relay(h, off, axis, d, piece, src=None):
        a, b = offset(h, off)
        key = (h, off, axis, d)
        send = gsem.at[FULL[key]] if piece is None else gpsem.at[PIECE[key]]
        u, v = off
        seen = ((u - d) % 4, v) if axis == 0 else (u, (v - d) % 4)
        ra, rb = offset(h, seen)
        k = h * 16 + ra * 4 + rb
        recv_ = bsem.at[k] if piece is None else bpsem.at[2 * k + piece]
        dst = rows(xall, a, b, h, piece)
        pltpu.make_async_remote_copy(src_ref=dst if src is None else src, dst_ref=dst, send_sem=send, recv_sem=recv_,
                                     device_id=neighbour(h, axis, d), device_id_type=MESH).start()

    def share(h, off, src=None):
        a, b = offset(h, off)
        dst = rows(xall, a, b, h, None)
        pltpu.make_async_remote_copy(
            src_ref=dst if src is None else src, dst_ref=dst, send_sem=hsem.at[h * 16 + a * 4 + b],
            recv_sem=dsem.at[a * 4 + b], device_id={'outer': mo, 'expert': 2 * mc + 1 - core},
            device_id_type=MESH).start()

    def other():
        return {'outer': mo, 'expert': 2 * mc + 1 - core}

    def arrive(ref, sem):
        pltpu.make_async_remote_copy(src_ref=ref, dst_ref=ref, send_sem=hsem.at[0], recv_sem=sem,
                                     device_id=other(), device_id_type=MESH).wait_recv()

    def event(h, off):
        a, b = offset(h, off)
        k = h * 16 + a * 4 + b
        if off[1] == 2 or off == (2, 0):
            for piece in range(2):
                arrive(rows(xall, a, b, h, piece), bpsem.at[2 * k + piece])
        else:
            arrive(rows(xall, a, b, h, None), bsem.at[k])
        for axis, d, piece in _relays(h, off):
            relay(h, off, axis, d, piece)
        share(h, off)

    def xcopy(s, slot):
        yd, xd, cd = dest(s)
        at = pl.ds(pl.multiple_of((yd * X + 2 * xd + cd) * T, T), T)
        return pltpu.make_async_copy(xall.at[at], xs.at[slot], xsem.at[slot])

    def xstart(s, slot):
        a, b = offs(s // 2)
        kk = lax.rem(s, 2)
        mine = (a + b + kk) == 0

        @pl.when(kk == 1)
        def _():
            yd, xd, cd = dest(s)
            at = pl.ds(pl.multiple_of((yd * X + 2 * xd + cd) * T, T), T)
            arrive(xall.at[at], dsem.at[a * 4 + b])

        @pl.when(mine)
        def _():
            pltpu.make_async_copy(x, xs.at[slot], xsem.at[slot]).start()

        @pl.when(jnp.logical_not(mine))
        def _():
            xcopy(s, slot).start()

    def send_a(s):
        yd, xd, cd = dest(s)
        return pltpu.make_async_remote_copy(
            src_ref=block(stage.at[0], yd * X + 2 * xd + cd), dst_ref=block(recv.at[0], at_a(yd, mx)),
            send_sem=ssem.at[0, s], recv_sem=rsem.at[0, s],
            device_id={'outer': mo, 'expert': 2 * xd + cd}, device_id_type=MESH)

    def send_b(s):
        yd, xd, cd = dest(s)
        return pltpu.make_async_remote_copy(
            src_ref=block(stage.at[1], yd * X + 2 * xd + cd), dst_ref=block(recv.at[1], at_b(xd, mo, core)),
            send_sem=ssem.at[1, s], recv_sem=rsem.at[1, s],
            device_id={'outer': yd, 'expert': 2 * mc + cd}, device_id_type=MESH)

    def away(s):
        a, b = offs(s // 2)
        k = lax.rem(s, 2)
        return b + k > 0, a + k > 0

    def experts(w1v, w3v, w2v, xt):
        def wcopies(e):
            return (pltpu.make_async_copy(w1.at[e], w1v.at[e], wsem.at[0, e]),
                    pltpu.make_async_copy(w3.at[e], w3v.at[e], wsem.at[1, e]),
                    pltpu.make_async_copy(w2.at[e], w2v.at[e], wsem.at[2, e]))

        pltpu.make_async_copy(x, xs.at[0], xsem.at[0]).start()
        pl.semaphore_wait(bar, n - 1)
        step = T // 2
        own = [x.at[pl.ds(h * step, step)] for h in range(2)]
        def spread(axis):
            for h in range(2):
                for d in NEAR:
                    relay(h, HERE, axis, d, None, own[h])

        spread(0)

        for e in range(el):
            for cp in wcopies(e):
                cp.start()
        pltpu.make_async_copy(x, xs.at[0], xsem.at[0]).wait()
        for i, table in enumerate(_tables(xs[0], wr[...], idx[...], C)):
            flat[:, :C] = table
            wide = jnp.concatenate([flat[pl.ds(e, n, stride=el), :][:, :C] for e in range(el)], axis=1)
            for m in range(n):
                pk[i, m // X, m % X] = wide[m:m + 1]
        tab_in[me] = pk[0, mo, mx]
        pk_a[mo] = pk[:, mo]
        pk_b[mc] = pk[:, :, pl.ds(2 * mc, 2)]
        for h in range(2):
            share(h, HERE, own[h])

        def tell(d, _):
            t = lax.rem(me + d, n)
            to, tx = t // X, lax.rem(t, X)
            pltpu.make_async_remote_copy(
                src_ref=pk.at[0, to, tx], dst_ref=tab_in.at[me], send_sem=tsem.at[0], recv_sem=tsem.at[1],
                device_id={'outer': to, 'expert': tx}, device_id_type=MESH).start()
            return 0

        lax.fori_loop(1, n, tell, 0)
        for d in range(1, O):
            for v in range(2):
                tsend(v, d).start()
        spread(1)
        tok = lax.broadcasted_iota(jnp.int32, (T, B), 0).astype(F32)

        for axis in range(2):
            for h in range(2):
                for d in NEAR:
                    event(h, (0, d) if axis else (d, 0))
        allrows = pltpu.make_async_remote_copy(
            src_ref=tab_in.at[pl.ds(0, n - 1)], dst_ref=tab_in.at[pl.ds(0, n - 1)], send_sem=tsem.at[0],
            recv_sem=tsem.at[1], device_id=other(), device_id_type=MESH)
        allrows.wait_recv()

        later = [(2, 0), (0, 2)] + [(u, v) for u in NEAR for v in NEAR]
        later += [(2, v) for v in NEAR] + [(u, 2) for u in NEAR] + [(2, 2)]
        plan = dict(zip(TIMES, later))

        xstart(0, 0)

        def group(g, _):
            def pick(j, _):
                s = g * G + j
                slot = lax.rem(s, 2)

                @pl.when(j + 1 < G)
                def _():
                    xstart(s + 1, 1 - slot)
                xcopy(s, slot).wait()
                yd, xd, cd = dest(s)
                row = tab_in[yd * X + 2 * xd + cd]
                hot = jnp.where(tok == row, 1.0, 0.0).astype(BF16)
                at = pl.ds(pl.multiple_of(j * C, C), C)
                for c0 in range(0, D, NT):
                    r = lax.dot_general(hot, xs[slot, :, c0:c0 + NT], (((0,), (0,)), ((), ())),
                                        preferred_element_type=F32).astype(BF16)
                    for e in range(el):
                        xt[e, at, c0:c0 + NT] = r[e * C:(e + 1) * C]
                return 0

            lax.fori_loop(0, G, pick, 0)

            def odrain(hh):
                for v in range(2):
                    pltpu.make_async_copy(ob.at[hh, :, pl.ds(v * H, H)], stage.at[v, pl.ds(0, half)],
                                          osem.at[hh, v]).wait()

            def ffn(e, _):
                hh = lax.rem(e, 2)

                @pl.when(g == 0)
                def _():
                    for cp in wcopies(e):
                        cp.wait()
                xr = xt[e]
                a = jnp.dot(xr, w1v[e], preferred_element_type=F32)
                b = jnp.dot(xr, w3v[e], preferred_element_type=F32)
                h = (jax.nn.silu(a) * b).astype(BF16)

                @pl.when(e >= 2)
                def _():
                    odrain(hh)
                for c0 in range(0, D, NT):
                    ob[hh, :, c0:c0 + NT] = jnp.dot(h, w2v[e, :, c0:c0 + NT],
                                                    preferred_element_type=F32).astype(BF16)
                for jj in range(G):
                    yd, xd, cd = dest(g * G + jj)
                    at = pl.ds(pl.multiple_of((yd * X + 2 * xd + cd) * B + e * C, C), C)
                    for v in range(2):
                        pltpu.make_async_copy(ob.at[hh, pl.ds(jj * C, C), pl.ds(v * H, H)],
                                              stage.at[v, at], osem.at[hh, v]).start()
                for t, todo in plan.items():
                    @pl.when(g * el + e == t)
                    def _(todo=todo):
                        for h in range(2):
                            event(h, todo)

                @pl.when((e == el - 2) & (g + 1 < NG))
                def _():
                    xstart((g + 1) * G, 0)
                return 0

            lax.fori_loop(0, el, ffn, 0)
            for hh in range(2):
                odrain(hh)

            def go(j, _):
                s = g * G + j
                far_a, far_b = away(s)

                @pl.when(far_a)
                def _():
                    send_a(s).start()

                @pl.when(far_b)
                def _():
                    send_b(s).start()
                return 0

            lax.fori_loop(0, G, go, 0)
            return 0

        lax.fori_loop(0, NG, group, 0)

    def tsend(v, d):
        yo, xo = lax.rem(mo + d, O), lax.rem(mc + d, W)
        if v == 0:
            src, dst, to = pk.at[:, yo], pk_a.at[mo], {'outer': yo, 'expert': mx}
        else:
            src, dst, to = pk.at[:, :, pl.ds(2 * xo, 2)], pk_b.at[mc], {'outer': mo, 'expert': 2 * xo + core}
        return pltpu.make_async_remote_copy(src_ref=src, dst_ref=dst, send_sem=tsem2.at[1 + v, d],
                                            recv_sem=tsem2.at[3 + v, d], device_id=to, device_id_type=MESH)

    pl.run_scoped(experts, pltpu.VMEM((el, D, FF), BF16), pltpu.VMEM((el, D, FF), BF16),
                  pltpu.VMEM((el, FF, D), BF16), pltpu.VMEM((el, half, D), BF16))

    for d in range(1, 4):
        tsend(0, d).wait()
        tsend(1, d).wait()

    def combine(pa, pb):
        pa[...] = jnp.zeros_like(pa)
        pb[...] = jnp.zeros_like(pb)
        tokf = lax.broadcasted_iota(jnp.int32, (T, 2 * B), 0).astype(F32)

        def origins(p):
            a, b = offs(p)
            return a, b, lax.rem(mo - a + O, O), lax.rem(mc - b + W, W)

        def fetch(p, slot):
            a, b, sy, sx = origins(p)
            yd, xd = lax.rem(mo + a, O), lax.rem(mc + b, W)
            for k in range(2):
                s = 2 * p + k
                c = lax.rem(core + k, 2)
                at = pl.ds(pl.multiple_of(c * B, B), B)
                for v in range(2):
                    if v == 0:
                        src, own = block(recv.at[0], at_a(yd, 2 * sx + c)), block(stage.at[0], yd * X + 2 * mc + core)
                    else:
                        src, own = block(recv.at[1], at_b(xd, sy, c)), block(stage.at[1], mo * X + 2 * xd + core)
                    far = (b if v == 0 else a) > 0

                    def bring(ref, v=v, at=at):
                        pltpu.make_async_copy(ref, xs.at[slot, at, pl.ds(v * H, H)], xsem.at[slot]).start()

                    def take(src=src, v=v, s=s, bring=bring):
                        pltpu.make_async_remote_copy(
                            src_ref=src, dst_ref=src, send_sem=ssem.at[v, s],
                            recv_sem=rsem.at[v, s],
                            device_id={'outer': mo, 'expert': lax.rem(mx + 1, X)},
                            device_id_type=MESH).wait_recv()
                        bring(src)
                    if k == 1:
                        take()
                    else:
                        pl.when(far)(take)
                        pl.when(jnp.logical_not(far))(functools.partial(bring, own))

        accs = (pa, pb)
        hr = T // 2
        pairs = [(v, r) for v in range(2) for r in range(2)]

        def late(r):
            return pl.ds(r * hr, hr)

        def psend(kind, v, r):
            d = NEAR[r]
            if kind == EARLY:
                src, dst = accs[v].at[d, late(1 - r)], part.at[v, r, late(1 - r)]
            elif kind == MID:
                src, dst = accs[v].at[2, late(r)], mid.at[v, r]
            else:
                src, dst = accs[v].at[d, late(r)], part.at[v, r, late(r)]
            if v == 0:
                to = {'outer': lax.rem(mo + d, O), 'expert': mx}
            else:
                to = {'outer': mo, 'expert': 2 * lax.rem(mc + d, W) + core}
            return pltpu.make_async_remote_copy(
                src_ref=src, dst_ref=dst, send_sem=pssem.at[kind, v, r], recv_sem=prsem.at[kind, v, r],
                device_id=to, device_id_type=MESH)

        fetch(0, 0)

        def weights(ref, d, r0):
            rows = [ref[(d, 0) + r0(c)] for c in range(2)]
            gs = [ref[(d, 1) + r0(c)] for c in range(2)]
            w = jnp.where(tokf == jnp.concatenate(rows, axis=1), jnp.concatenate(gs, axis=1), 0.0)
            return _split(w)

        def comb(p, _):
            slot = lax.rem(p, 2)

            @pl.when(p + 1 < n // 2)
            def _():
                fetch(p + 1, 1 - slot)
            a, b, sy, sx = origins(p)
            wa = weights(pk_a, lax.rem(mo + a, O), lambda c: (2 * sx + c,))
            wb = weights(pk_b, lax.rem(mc + b, W), lambda c: (sy, c))
            pltpu.make_async_copy(xall.at[pl.ds(0, T)], xs.at[slot], xsem.at[slot]).wait()
            for acc, d, ws, base in ((pa, a, wa, 0), (pb, b, wb, H)):
                for c0 in range(0, H, NT):
                    rr = xs[slot, :, base + c0:base + c0 + NT]
                    acc[d, :, c0:c0 + NT] += (jnp.dot(ws[0], rr, preferred_element_type=F32)
                                              + jnp.dot(ws[1], rr, preferred_element_type=F32)
                                              + jnp.dot(ws[2], rr, preferred_element_type=F32))
            for last, kind, sides in ((11, EARLY, pairs[:2]), (13, EARLY, pairs[2:]), (15, MID, pairs)):
                @pl.when(p == last)
                def _(kind=kind, sides=sides):
                    for v, r in sides:
                        psend(kind, v, r).start()
            return 0

        lax.fori_loop(0, n // 2, comb, 0)

        def land(v, r, half_):
            return pltpu.make_async_copy(part.at[v, r, late(half_)], accs[v].at[NEAR[r], late(half_)], psem.at[v, r])

        for v, r in pairs:
            psend(EARLY, v, r).wait()
            land(v, r, 1 - r).start()
        for v, r in pairs:
            land(v, r, 1 - r).wait()
            accs[v][0, late(1 - r)] += accs[v][NEAR[r], late(1 - r)]
        for v, r in pairs:
            psend(MID, v, r).wait()
            accs[v][NEAR[r], late(r)] += mid[v, r]
            psend(LATE, v, r).start()

        def sent(s, _):
            far_a, far_b = away(s)

            @pl.when(far_a)
            def _():
                send_a(s).wait_send()

            @pl.when(far_b)
            def _():
                send_b(s).wait_send()
            return 0

        lax.fori_loop(0, n, sent, 0)

        def wsend(ref, sem):
            pltpu.make_async_remote_copy(src_ref=ref, dst_ref=ref, send_sem=sem, recv_sem=tsem.at[1],
                                         device_id=other(), device_id_type=MESH).wait_send()

        def gone(i, _):
            wsend(xall.at[pl.ds(0, T // 2)], gsem.at[i])
            return 0

        lax.fori_loop(0, len(FULL), gone, 0)

        def gonep(i, _):
            wsend(xall.at[pl.ds(0, T // 4)], gpsem.at[i])
            return 0

        lax.fori_loop(0, len(PIECE), gonep, 0)

        def goneh(i, _):
            wsend(xall.at[pl.ds(0, T // 2)], hsem.at[i])
            return 0

        lax.fori_loop(0, n, goneh, 0)
        wsend(tab_in.at[pl.ds(0, n - 1)], tsem.at[0])

        for v, r in pairs:
            psend(LATE, v, r).wait()
            land(v, r, r).start()
        for v, r in pairs:
            land(v, r, r).wait()
            ob[r, :, v * H:(v + 1) * H] = (accs[v][0, late(r)] + accs[v][NEAR[r], late(r)]).astype(BF16)
        cps = [pltpu.make_async_copy(ob.at[hh], y.at[pl.ds(hh * half, half)], osem.at[hh, 0])
               for hh in range(T // half)]
        for cp in cps:
            cp.start()
        for cp in cps:
            cp.wait()

    pl.run_scoped(combine, pltpu.VMEM((O, T, H), F32), pltpu.VMEM((W, T, H), F32))


def solution(mesh):
    O = mesh.shape['outer']
    X = mesh.shape['expert']
    n = O * X
    tok = P(('data', 'outer', 'expert'), None)
    wsp = P(('outer', 'expert'), None, None)

    def local(x, wr, idx, w1, w3, w2):
        T, D = x.shape
        k = idx.shape[1]
        E = wr.shape[1]
        el, _, FF = w1.shape
        C = 2 * T * k // E
        B = el * C
        anyspec = pl.BlockSpec(memory_space=pl.ANY)
        vspec = pl.BlockSpec(memory_space=pltpu.VMEM)
        y = pl.pallas_call(
            functools.partial(_kernel, O, X, el, C),
            out_shape=(jax.ShapeDtypeStruct((T, D), BF16),
                       jax.ShapeDtypeStruct((n * T, D), BF16),
                       jax.ShapeDtypeStruct((2, n * B, D // 2), BF16),
                       jax.ShapeDtypeStruct((2, n * B, D // 2), BF16),
                       jax.ShapeDtypeStruct((2, 2, T, D // 2), F32)),
            in_specs=[anyspec, vspec, vspec, anyspec, anyspec, anyspec],
            out_specs=(anyspec,) * 5,
            scratch_shapes=[
                pltpu.VMEM((2, T, D), BF16),
                pltpu.VMEM((2, 4 * C, D), BF16),
                pltpu.VMEM((2, O, X, 1, B), F32),
                pltpu.VMEM((E, E), F32),
                pltpu.VMEM((n, 1, B), F32),
                pltpu.VMEM((O, 2, X, 1, B), F32),
                pltpu.VMEM((X // 2, 2, O, 2, 1, B), F32),
                pltpu.VMEM((2, 2, T // 2, D // 2), F32),
                pltpu.SemaphoreType.DMA((3, el)),
                pltpu.SemaphoreType.DMA((2,)),
                pltpu.SemaphoreType.DMA((2, 2)),
                pltpu.SemaphoreType.DMA((2, n)),
                pltpu.SemaphoreType.DMA((2, n)),
                pltpu.SemaphoreType.DMA((3, 2, 2)),
                pltpu.SemaphoreType.DMA((3, 2, 2)),
                pltpu.SemaphoreType.DMA((2, 2)),
                pltpu.SemaphoreType.DMA((32,)),
                pltpu.SemaphoreType.DMA((64,)),
                pltpu.SemaphoreType.DMA((32,)),
                pltpu.SemaphoreType.DMA((32,)),
                pltpu.SemaphoreType.DMA((16,)),
                pltpu.SemaphoreType.DMA((32,)),
                pltpu.SemaphoreType.DMA((2,)),
                pltpu.SemaphoreType.DMA((5, 4)),
            ],
            compiler_params=pltpu.CompilerParams(
                collective_id=0, has_side_effects=True, vmem_limit_bytes=67043328),
        )(x, wr, idx, w1, w3, w2)
        return y[0]

    return jax.shard_map(local, mesh=mesh, in_specs=(tok, P(None, None), tok, wsp, wsp, wsp), out_specs=tok, check_vma=False)
```

```python
import functools

import jax
import jax.numpy as jnp
from jax import lax
from jax.experimental import pallas as pl
from jax.experimental.pallas import tpu as pltpu
from jax.sharding import PartitionSpec as P

MESH = pl.DeviceIdType.MESH
F32 = jnp.float32
BF16 = jnp.bfloat16


def _split(w):
    hi = w.astype(BF16)
    r = w - hi.astype(F32)
    mid = r.astype(BF16)
    return hi, mid, (r - mid.astype(F32)).astype(BF16)


def _tables(xv, wr, idx, C):
    T, k = idx.shape
    E = wr.shape[1]
    logits = jnp.dot(xv, wr, preferred_element_type=F32)
    lane = lax.broadcasted_iota(jnp.int32, (T, E), 1)
    hits = [idx[:, j:j + 1] == lane for j in range(k)]

    def take(table):
        return [jnp.sum(jnp.where(h, table, 0.0), axis=1, keepdims=True) for h in hits]

    at = take(logits)
    top = functools.reduce(jnp.maximum, at)
    ex = [jnp.exp(v - top) for v in at]
    tot = functools.reduce(jnp.add, ex)
    ones = [jnp.where(h, 1.0, 0.0) for h in hits]
    many = functools.reduce(jnp.add, ones).astype(BF16)
    tri = lax.broadcasted_iota(jnp.int32, (T, T), 1) < lax.broadcasted_iota(jnp.int32, (T, T), 0)
    rank = take(jnp.dot(jnp.where(tri, 1.0, 0.0).astype(BF16), many, preferred_element_type=F32))
    slot = lax.rem(lane, C).astype(F32)
    left = lane < C
    tok = lax.broadcasted_iota(jnp.int32, (T, 1), 0) + 1
    lo = lax.rem(tok, T // 2).astype(F32)
    hi = (tok // (T // 2)).astype(F32)
    res = [0.0] * 3
    for j in range(k):
        g = [v.astype(F32) for v in _split(ex[j] / tot)]
        hot = ones[j].astype(BF16)
        here = rank[j] == slot
        for i, (u, v) in enumerate(((hi, lo), (g[0], g[1]), (g[2], g[2]))):
            val = jnp.where(here, jnp.where(left, u, v), 0.0).astype(BF16)
            res[i] += lax.dot_general(hot, val, (((0,), (0,)), ((), ())), preferred_element_type=F32)
    tab = res[0][:, :C] * (T // 2) + res[0][:, C:2 * C] - 1.0
    return tab, (res[1][:, :C] + res[1][:, C:2 * C]) + res[2][:, :C]


ORDER = ((0, 1), (0, 3), (1, 0), (3, 0), (2, 0), (0, 2), (1, 1), (3, 3),
         (1, 3), (3, 1), (1, 2), (3, 2), (2, 1), (2, 3), (0, 0), (2, 2))
NEAR = (1, 3)
EARLY, MID, LATE = range(3)
HERE = (0, 0)
TIMES = (0, 1, 3, 4, 5, 6, 8, 9, 10, 11, 22)


def _lut(vals, i):
    r = vals[0]
    for k in range(1, len(vals)):
        r = jnp.where(i == k, vals[k], r)
    return r


def _relays(h, off):
    u, v = off
    if v == 0:
        if u == 3:
            return ((0, 1, 0), (1, 1, None), (1, 3, None))
        if u == 1:
            return ((0, 3, 1), (1, 1, None), (1, 3, None))
        return ((1, 1, None), (1, 3, None))
    if v == 3:
        return ((1, 1, 0),)
    if v == 1:
        return ((1, 3, 1),)
    return ()


def _numbered():
    full, piece = {}, {}
    for h in range(2):
        for d in NEAR:
            for axis in range(2):
                full[(h, HERE, axis, d)] = len(full)
        for off in ORDER:
            if off != HERE:
                for axis, d, part in _relays(h, off):
                    table = full if part is None else piece
                    table[(h, off, axis, d)] = len(table)
    return full, piece


FULL, PIECE = _numbered()


def _kernel(O, X, el, C, x, wr, idx, w1, w3, w2, y, xall, stage, recv, part,
            xs, ob, pk, flat, tab_in, pk_a, pk_b, mid, wsem, xsem, osem, ssem, rsem, pssem, prsem, psem,
            bsem, bpsem, gsem, gpsem, dsem, hsem, tsem, tsem2):
    n = O * X
    W = X // 2
    _, T, D = xs.shape
    H = D // 2
    FF = w1.shape[2]
    B = el * C
    G = 4
    NG = n // G
    half = G * C
    NT = 512
    mo = lax.axis_index('outer')
    mx = lax.axis_index('expert')
    mc = mx // 2
    core = lax.rem(mx, 2)
    me = mo * X + mx

    def offs(p):
        return _lut([o[0] for o in ORDER], p), _lut([o[1] for o in ORDER], p)

    def dest(s):
        a, b = offs(s // 2)
        return lax.rem(mo + a, O), lax.rem(mc + b, W), lax.rem(core + lax.rem(s, 2), 2)

    def block(ref, d):
        return ref.at[pl.ds(pl.multiple_of(d * B, B), B)]

    def at_a(yd, sx):
        return yd * X + sx

    def at_b(xd, sy, sc):
        return xd * X + sy * 2 + sc

    bar = pltpu.get_barrier_semaphore()

    def greet(d, _):
        t = lax.rem(me + d, n)
        pl.semaphore_signal(bar, inc=1, device_id={'outer': t // X, 'expert': lax.rem(t, X)}, device_id_type=MESH)
        return 0

    lax.fori_loop(1, n, greet, 0)

    def rows(ref, a, b, h, piece, c=None):
        src = lax.rem(mo + a, O) * X + 2 * lax.rem(mc + b, W) + (core if c is None else c)
        step = T // 2
        if piece is None:
            return ref.at[pl.ds(pl.multiple_of(src * T + h * step, step), step)]
        return ref.at[pl.ds(pl.multiple_of(src * T + h * step + piece * (step // 2), step // 2), step // 2)]

    def neighbour(h, axis, d):
        if (axis == 0) == (h == 0):
            return {'outer': mo, 'expert': 2 * lax.rem(mc + d, W) + core}
        return {'outer': lax.rem(mo + d, O), 'expert': mx}

    def offset(h, off):
        return (off[1], off[0]) if h == 0 else off

    def relay(h, off, axis, d, piece, src=None):
        a, b = offset(h, off)
        key = (h, off, axis, d)
        send = gsem.at[FULL[key]] if piece is None else gpsem.at[PIECE[key]]
        u, v = off
        seen = ((u - d) % 4, v) if axis == 0 else (u, (v - d) % 4)
        ra, rb = offset(h, seen)
        k = h * 16 + ra * 4 + rb
        recv_ = bsem.at[k] if piece is None else bpsem.at[2 * k + piece]
        dst = rows(xall, a, b, h, piece)
        pltpu.make_async_remote_copy(src_ref=dst if src is None else src, dst_ref=dst, send_sem=send, recv_sem=recv_,
                                     device_id=neighbour(h, axis, d), device_id_type=MESH).start()

    def share(h, off, src=None):
        a, b = offset(h, off)
        dst = rows(xall, a, b, h, None)
        pltpu.make_async_remote_copy(
            src_ref=dst if src is None else src, dst_ref=dst, send_sem=hsem.at[h * 16 + a * 4 + b],
            recv_sem=dsem.at[a * 4 + b], device_id={'outer': mo, 'expert': 2 * mc + 1 - core},
            device_id_type=MESH).start()

    def other():
        return {'outer': mo, 'expert': 2 * mc + 1 - core}

    def arrive(ref, sem):
        pltpu.make_async_remote_copy(src_ref=ref, dst_ref=ref, send_sem=hsem.at[0], recv_sem=sem,
                                     device_id=other(), device_id_type=MESH).wait_recv()

    def event(h, off):
        a, b = offset(h, off)
        k = h * 16 + a * 4 + b
        if off[1] == 2 or off == (2, 0):
            for piece in range(2):
                arrive(rows(xall, a, b, h, piece), bpsem.at[2 * k + piece])
        else:
            arrive(rows(xall, a, b, h, None), bsem.at[k])
        for axis, d, piece in _relays(h, off):
            relay(h, off, axis, d, piece)
        share(h, off)

    def xcopy(s, slot):
        yd, xd, cd = dest(s)
        at = pl.ds(pl.multiple_of((yd * X + 2 * xd + cd) * T, T), T)
        return pltpu.make_async_copy(xall.at[at], xs.at[slot], xsem.at[slot])

    def xstart(s, slot):
        a, b = offs(s // 2)
        kk = lax.rem(s, 2)
        mine = (a + b + kk) == 0

        @pl.when(kk == 1)
        def _():
            yd, xd, cd = dest(s)
            at = pl.ds(pl.multiple_of((yd * X + 2 * xd + cd) * T, T), T)
            arrive(xall.at[at], dsem.at[a * 4 + b])

        @pl.when(mine)
        def _():
            pltpu.make_async_copy(x, xs.at[slot], xsem.at[slot]).start()

        @pl.when(jnp.logical_not(mine))
        def _():
            xcopy(s, slot).start()

    def send_a(s):
        yd, xd, cd = dest(s)
        return pltpu.make_async_remote_copy(
            src_ref=block(stage.at[0], yd * X + 2 * xd + cd), dst_ref=block(recv.at[0], at_a(yd, mx)),
            send_sem=ssem.at[0, s], recv_sem=rsem.at[0, s],
            device_id={'outer': mo, 'expert': 2 * xd + cd}, device_id_type=MESH)

    def send_b(s):
        yd, xd, cd = dest(s)
        return pltpu.make_async_remote_copy(
            src_ref=block(stage.at[1], yd * X + 2 * xd + cd), dst_ref=block(recv.at[1], at_b(xd, mo, core)),
            send_sem=ssem.at[1, s], recv_sem=rsem.at[1, s],
            device_id={'outer': yd, 'expert': 2 * mc + cd}, device_id_type=MESH)

    def away(s):
        a, b = offs(s // 2)
        k = lax.rem(s, 2)
        return b + k > 0, a + k > 0

    def experts(w1v, w3v, w2v, xt):
        def wcopies(e):
            return (pltpu.make_async_copy(w1.at[e], w1v.at[e], wsem.at[0, e]),
                    pltpu.make_async_copy(w3.at[e], w3v.at[e], wsem.at[1, e]),
                    pltpu.make_async_copy(w2.at[e], w2v.at[e], wsem.at[2, e]))

        pltpu.make_async_copy(x, xs.at[0], xsem.at[0]).start()
        pl.semaphore_wait(bar, n - 1)
        step = T // 2
        own = [x.at[pl.ds(h * step, step)] for h in range(2)]
        def spread(axis):
            for h in range(2):
                for d in NEAR:
                    relay(h, HERE, axis, d, None, own[h])

        spread(0)

        for e in range(el):
            for cp in wcopies(e):
                cp.start()
        pltpu.make_async_copy(x, xs.at[0], xsem.at[0]).wait()
        for i, table in enumerate(_tables(xs[0], wr[...], idx[...], C)):
            flat[:, :C] = table
            wide = jnp.concatenate([flat[pl.ds(e, n, stride=el), :][:, :C] for e in range(el)], axis=1)
            for m in range(n):
                pk[i, m // X, m % X] = wide[m:m + 1]
        tab_in[me] = pk[0, mo, mx]
        pk_a[mo] = pk[:, mo]
        pk_b[mc] = pk[:, :, pl.ds(2 * mc, 2)]
        for h in range(2):
            share(h, HERE, own[h])

        def tell(d, _):
            t = lax.rem(me + d, n)
            to, tx = t // X, lax.rem(t, X)
            pltpu.make_async_remote_copy(
                src_ref=pk.at[0, to, tx], dst_ref=tab_in.at[me], send_sem=tsem.at[0], recv_sem=tsem.at[1],
                device_id={'outer': to, 'expert': tx}, device_id_type=MESH).start()
            return 0

        lax.fori_loop(1, n, tell, 0)
        for d in range(1, O):
            for v in range(2):
                tsend(v, d).start()
        spread(1)
        tok = lax.broadcasted_iota(jnp.int32, (T, B), 0).astype(F32)

        for axis in range(2):
            for h in range(2):
                for d in NEAR:
                    event(h, (0, d) if axis else (d, 0))
        allrows = pltpu.make_async_remote_copy(
            src_ref=tab_in.at[pl.ds(0, n - 1)], dst_ref=tab_in.at[pl.ds(0, n - 1)], send_sem=tsem.at[0],
            recv_sem=tsem.at[1], device_id=other(), device_id_type=MESH)
        allrows.wait_recv()

        later = [(2, 0), (0, 2)] + [(u, v) for u in NEAR for v in NEAR]
        later += [(2, v) for v in NEAR] + [(u, 2) for u in NEAR] + [(2, 2)]
        plan = dict(zip(TIMES, later))

        xstart(0, 0)

        def group(g, _):
            def pick(j, _):
                s = g * G + j
                slot = lax.rem(s, 2)

                @pl.when(j + 1 < G)
                def _():
                    xstart(s + 1, 1 - slot)
                xcopy(s, slot).wait()
                yd, xd, cd = dest(s)
                row = tab_in[yd * X + 2 * xd + cd]
                hot = jnp.where(tok == row, 1.0, 0.0).astype(BF16)
                at = pl.ds(pl.multiple_of(j * C, C), C)
                for c0 in range(0, D, NT):
                    r = lax.dot_general(hot, xs[slot, :, c0:c0 + NT], (((0,), (0,)), ((), ())),
                                        preferred_element_type=F32).astype(BF16)
                    for e in range(el):
                        xt[e, at, c0:c0 + NT] = r[e * C:(e + 1) * C]
                return 0

            lax.fori_loop(0, G, pick, 0)

            def odrain(hh):
                for v in range(2):
                    pltpu.make_async_copy(ob.at[hh, :, pl.ds(v * H, H)], stage.at[v, pl.ds(0, half)],
                                          osem.at[hh, v]).wait()

            def ffn(e, _):
                hh = lax.rem(e, 2)

                @pl.when(g == 0)
                def _():
                    for cp in wcopies(e):
                        cp.wait()
                xr = xt[e]
                a = jnp.dot(xr, w1v[e], preferred_element_type=F32)
                b = jnp.dot(xr, w3v[e], preferred_element_type=F32)
                h = (jax.nn.silu(a) * b).astype(BF16)

                @pl.when(e >= 2)
                def _():
                    odrain(hh)
                for c0 in range(0, D, NT):
                    ob[hh, :, c0:c0 + NT] = jnp.dot(h, w2v[e, :, c0:c0 + NT],
                                                    preferred_element_type=F32).astype(BF16)
                for jj in range(G):
                    yd, xd, cd = dest(g * G + jj)
                    at = pl.ds(pl.multiple_of((yd * X + 2 * xd + cd) * B + e * C, C), C)
                    for v in range(2):
                        pltpu.make_async_copy(ob.at[hh, pl.ds(jj * C, C), pl.ds(v * H, H)],
                                              stage.at[v, at], osem.at[hh, v]).start()
                for t, todo in plan.items():
                    @pl.when(g * el + e == t)
                    def _(todo=todo):
                        for h in range(2):
                            event(h, todo)

                @pl.when((e == el - 2) & (g + 1 < NG))
                def _():
                    xstart((g + 1) * G, 0)
                return 0

            lax.fori_loop(0, el, ffn, 0)
            for hh in range(2):
                odrain(hh)

            def go(j, _):
                s = g * G + j
                far_a, far_b = away(s)

                @pl.when(far_a)
                def _():
                    send_a(s).start()

                @pl.when(far_b)
                def _():
                    send_b(s).start()
                return 0

            lax.fori_loop(0, G, go, 0)
            return 0

        lax.fori_loop(0, NG, group, 0)

    def tsend(v, d):
        yo, xo = lax.rem(mo + d, O), lax.rem(mc + d, W)
        if v == 0:
            src, dst, to = pk.at[:, yo], pk_a.at[mo], {'outer': yo, 'expert': mx}
        else:
            src, dst, to = pk.at[:, :, pl.ds(2 * xo, 2)], pk_b.at[mc], {'outer': mo, 'expert': 2 * xo + core}
        return pltpu.make_async_remote_copy(src_ref=src, dst_ref=dst, send_sem=tsem2.at[1 + v, d],
                                            recv_sem=tsem2.at[3 + v, d], device_id=to, device_id_type=MESH)

    pl.run_scoped(experts, pltpu.VMEM((el, D, FF), BF16), pltpu.VMEM((el, D, FF), BF16),
                  pltpu.VMEM((el, FF, D), BF16), pltpu.VMEM((el, half, D), BF16))

    for d in range(1, 4):
        tsend(0, d).wait()
        tsend(1, d).wait()

    def combine(pa, pb):
        pa[...] = jnp.zeros_like(pa)
        pb[...] = jnp.zeros_like(pb)
        tokf = lax.broadcasted_iota(jnp.int32, (T, 2 * B), 0).astype(F32)

        def origins(p):
            a, b = offs(p)
            return a, b, lax.rem(mo - a + O, O), lax.rem(mc - b + W, W)

        def fetch(p, slot):
            a, b, sy, sx = origins(p)
            yd, xd = lax.rem(mo + a, O), lax.rem(mc + b, W)
            for k in range(2):
                s = 2 * p + k
                c = lax.rem(core + k, 2)
                at = pl.ds(pl.multiple_of(c * B, B), B)
                for v in range(2):
                    if v == 0:
                        src, own = block(recv.at[0], at_a(yd, 2 * sx + c)), block(stage.at[0], yd * X + 2 * mc + core)
                    else:
                        src, own = block(recv.at[1], at_b(xd, sy, c)), block(stage.at[1], mo * X + 2 * xd + core)
                    far = (b if v == 0 else a) > 0

                    def bring(ref, v=v, at=at):
                        pltpu.make_async_copy(ref, xs.at[slot, at, pl.ds(v * H, H)], xsem.at[slot]).start()

                    def take(src=src, v=v, s=s, bring=bring):
                        pltpu.make_async_remote_copy(
                            src_ref=src, dst_ref=src, send_sem=ssem.at[v, s],
                            recv_sem=rsem.at[v, s],
                            device_id={'outer': mo, 'expert': lax.rem(mx + 1, X)},
                            device_id_type=MESH).wait_recv()
                        bring(src)
                    if k == 1:
                        take()
                    else:
                        pl.when(far)(take)
                        pl.when(jnp.logical_not(far))(functools.partial(bring, own))

        accs = (pa, pb)
        hr = T // 2
        pairs = [(v, r) for v in range(2) for r in range(2)]

        def late(r):
            return pl.ds(r * hr, hr)

        def psend(kind, v, r):
            d = NEAR[r]
            if kind == EARLY:
                src, dst = accs[v].at[d, late(1 - r)], part.at[v, r, late(1 - r)]
            elif kind == MID:
                src, dst = accs[v].at[2, late(r)], mid.at[v, r]
            else:
                src, dst = accs[v].at[d, late(r)], part.at[v, r, late(r)]
            if v == 0:
                to = {'outer': lax.rem(mo + d, O), 'expert': mx}
            else:
                to = {'outer': mo, 'expert': 2 * lax.rem(mc + d, W) + core}
            return pltpu.make_async_remote_copy(
                src_ref=src, dst_ref=dst, send_sem=pssem.at[kind, v, r], recv_sem=prsem.at[kind, v, r],
                device_id=to, device_id_type=MESH)

        fetch(0, 0)

        def weights(ref, d, r0):
            rows = [ref[(d, 0) + r0(c)] for c in range(2)]
            gs = [ref[(d, 1) + r0(c)] for c in range(2)]
            w = jnp.where(tokf == jnp.concatenate(rows, axis=1), jnp.concatenate(gs, axis=1), 0.0)
            return _split(w)

        def comb(p, _):
            slot = lax.rem(p, 2)

            @pl.when(p + 1 < n // 2)
            def _():
                fetch(p + 1, 1 - slot)
            a, b, sy, sx = origins(p)
            wa = weights(pk_a, lax.rem(mo + a, O), lambda c: (2 * sx + c,))
            wb = weights(pk_b, lax.rem(mc + b, W), lambda c: (sy, c))
            pltpu.make_async_copy(xall.at[pl.ds(0, T)], xs.at[slot], xsem.at[slot]).wait()
            for acc, d, ws, base in ((pa, a, wa, 0), (pb, b, wb, H)):
                for c0 in range(0, H, NT):
                    rr = xs[slot, :, base + c0:base + c0 + NT]
                    acc[d, :, c0:c0 + NT] += (jnp.dot(ws[0], rr, preferred_element_type=F32)
                                              + jnp.dot(ws[1], rr, preferred_element_type=F32)
                                              + jnp.dot(ws[2], rr, preferred_element_type=F32))
            for last, kind, sides in ((11, EARLY, pairs[:2]), (13, EARLY, pairs[2:]), (15, MID, pairs)):
                @pl.when(p == last)
                def _(kind=kind, sides=sides):
                    for v, r in sides:
                        psend(kind, v, r).start()
            return 0

        lax.fori_loop(0, n // 2, comb, 0)

        def land(v, r, half_):
            return pltpu.make_async_copy(part.at[v, r, late(half_)], accs[v].at[NEAR[r], late(half_)], psem.at[v, r])

        for v, r in pairs:
            psend(EARLY, v, r).wait()
            land(v, r, 1 - r).start()
        for v, r in pairs:
            land(v, r, 1 - r).wait()
            accs[v][0, late(1 - r)] += accs[v][NEAR[r], late(1 - r)]
        for v, r in pairs:
            psend(MID, v, r).wait()
            accs[v][NEAR[r], late(r)] += mid[v, r]
            psend(LATE, v, r).start()

        def sent(s, _):
            far_a, far_b = away(s)

            @pl.when(far_a)
            def _():
                send_a(s).wait_send()

            @pl.when(far_b)
            def _():
                send_b(s).wait_send()
            return 0

        lax.fori_loop(0, n, sent, 0)

        def wsend(ref, sem):
            pltpu.make_async_remote_copy(src_ref=ref, dst_ref=ref, send_sem=sem, recv_sem=tsem.at[1],
                                         device_id=other(), device_id_type=MESH).wait_send()

        def gone(i, _):
            wsend(xall.at[pl.ds(0, T // 2)], gsem.at[i])
            return 0

        lax.fori_loop(0, len(FULL), gone, 0)

        def gonep(i, _):
            wsend(xall.at[pl.ds(0, T // 4)], gpsem.at[i])
            return 0

        lax.fori_loop(0, len(PIECE), gonep, 0)

        def goneh(i, _):
            wsend(xall.at[pl.ds(0, T // 2)], hsem.at[i])
            return 0

        lax.fori_loop(0, n, goneh, 0)
        wsend(tab_in.at[pl.ds(0, n - 1)], tsem.at[0])

        for v, r in pairs:
            psend(LATE, v, r).wait()
            land(v, r, r).start()
        for v, r in pairs:
            land(v, r, r).wait()
            ob[r, :, v * H:(v + 1) * H] = (accs[v][0, late(r)] + accs[v][NEAR[r], late(r)]).astype(BF16)
        cps = [pltpu.make_async_copy(ob.at[hh], y.at[pl.ds(hh * half, half)], osem.at[hh, 0])
               for hh in range(T // half)]
        for cp in cps:
            cp.start()
        for cp in cps:
            cp.wait()

    pl.run_scoped(combine, pltpu.VMEM((O, T, H), F32), pltpu.VMEM((W, T, H), F32))


def solution(mesh):
    O = mesh.shape['outer']
    X = mesh.shape['expert']
    n = O * X
    tok = P(('data', 'outer', 'expert'), None)
    wsp = P(('outer', 'expert'), None, None)

    def local(x, wr, idx, w1, w3, w2):
        T, D = x.shape
        k = idx.shape[1]
        E = wr.shape[1]
        el, _, FF = w1.shape
        C = 2 * T * k // E
        B = el * C
        anyspec = pl.BlockSpec(memory_space=pl.ANY)
        vspec = pl.BlockSpec(memory_space=pltpu.VMEM)
        y = pl.pallas_call(
            functools.partial(_kernel, O, X, el, C),
            out_shape=(jax.ShapeDtypeStruct((T, D), BF16),
                       jax.ShapeDtypeStruct((n * T, D), BF16),
                       jax.ShapeDtypeStruct((2, n * B, D // 2), BF16),
                       jax.ShapeDtypeStruct((2, n * B, D // 2), BF16),
                       jax.ShapeDtypeStruct((2, 2, T, D // 2), F32)),
            in_specs=[anyspec, vspec, vspec, anyspec, anyspec, anyspec],
            out_specs=(anyspec,) * 5,
            scratch_shapes=[
                pltpu.VMEM((2, T, D), BF16),
                pltpu.VMEM((2, 4 * C, D), BF16),
                pltpu.VMEM((2, O, X, 1, B), F32),
                pltpu.VMEM((E, E), F32),
                pltpu.VMEM((n, 1, B), F32),
                pltpu.VMEM((O, 2, X, 1, B), F32),
                pltpu.VMEM((X // 2, 2, O, 2, 1, B), F32),
                pltpu.VMEM((2, 2, T // 2, D // 2), F32),
                pltpu.SemaphoreType.DMA((3, el)),
                pltpu.SemaphoreType.DMA((2,)),
                pltpu.SemaphoreType.DMA((2, 2)),
                pltpu.SemaphoreType.DMA((2, n)),
                pltpu.SemaphoreType.DMA((2, n)),
                pltpu.SemaphoreType.DMA((3, 2, 2)),
                pltpu.SemaphoreType.DMA((3, 2, 2)),
                pltpu.SemaphoreType.DMA((2, 2)),
                pltpu.SemaphoreType.DMA((32,)),
                pltpu.SemaphoreType.DMA((64,)),
                pltpu.SemaphoreType.DMA((32,)),
                pltpu.SemaphoreType.DMA((32,)),
                pltpu.SemaphoreType.DMA((16,)),
                pltpu.SemaphoreType.DMA((32,)),
                pltpu.SemaphoreType.DMA((2,)),
                pltpu.SemaphoreType.DMA((5, 4)),
            ],
            compiler_params=pltpu.CompilerParams(
                collective_id=0, has_side_effects=True, vmem_limit_bytes=67043328),
        )(x, wr, idx, w1, w3, w2)
        return y[0]

    return jax.shard_map(local, mesh=mesh, in_specs=(tok, P(None, None), tok, wsp, wsp, wsp), out_specs=tok, check_vma=False)
```
